32 devices in a mesh: dp: 16 (over z, x, core), tensor: 2 (over y).
Axes of the slice: x: 2, y: 2, z: 4, core: 2. Of those that a mesh axis runs over, the one named last changes fastest.
Arguments:
- drafter_hidden: bfloat16 [2, 2048, 4096], P(None, 'dp', 'tensor'), may hold values from -2000 to 2000
- norm_gain: bfloat16 [4096], P('tensor'), may hold values from 0.5 to 1.5
- head_weight: bfloat16 [4096, 8192], P('tensor', 'dp'), may hold values from -24 to 24
- labels: int32 [2048], P('dp'), may hold values from 0 to 8191
- loss_mask: int32 [2048], P('dp'), may hold values 0 or 1
- offsets: int32 [2], replicated, may hold values from 1 to 4
Outputs:
- draft_loss: float32 [], replicated
- head_grad: float32 [4096, 8192], P('tensor', 'dp')
The draws below stay inside these ranges and needn't reach their ends.
All inputs are finite; a program needn't handle non-finite values. No bound on the sum of `loss_mask` on one device may be relied on, other than what follows from the above.
Results may differ from the reference program's by a relative error of at most 0.0048.
Values may be sent and summed in bfloat16 or wider, within the bound.
A program may use at most 128 MiB of HBM per device.

```python
import math
import jax
import jax.numpy as jnp
from jax import lax

D = 4096
STEPS = 2
WINDOW = 512
MAXOFF = 4
TOKENS = 2048
VOCAB = 8192


def shared_head(key):
    head_key = jax.random.fold_in(key, 11)
    values = jax.random.truncated_normal(head_key, -6.0, 6.0, (D, VOCAB), jnp.float32)
    loud = max(1.0, 48.0 / math.sqrt(D))
    column_ids = jnp.arange(VOCAB)
    boost = jnp.where(column_ids % 8 == 3, loud, 1.0).astype(jnp.float32)
    return values * (5.0 / math.sqrt(D)) * boost[None, :]


def draw_head_weight(key, part):
    return shared_head(key).astype(jnp.bfloat16)


def draw_drafter_hidden(key, part):
    noise_key = jax.random.fold_in(key, 21)
    scale_key = jax.random.fold_in(key, 22)
    first_key = jax.random.fold_in(key, 24)
    second_key = jax.random.fold_in(key, 25)
    noise = jax.random.truncated_normal(noise_key, -6.0, 6.0, (STEPS, TOKENS, D), jnp.float32)
    row_scale = jnp.exp(jax.random.uniform(scale_key, (STEPS, TOKENS, 1), jnp.float32, 0.0, math.log(10.0)))
    head_rows = shared_head(key).T
    groups = VOCAB // 8
    first = 8 * jax.random.randint(first_key, (STEPS, TOKENS), 0, groups) + 3
    second = (first + 8 * jax.random.randint(second_key, (STEPS, TOKENS), 1, groups)) % VOCAB
    positions = jnp.arange(TOKENS)
    chosen = (positions % 61 == 7)[None, :, None]
    strengths = jnp.array([0.5, 1.0, 2.0, 3.0], jnp.float32)[positions // 61 % 4][None, :, None]
    signal = strengths * 8.0 * (head_rows[first] + 0.99 * head_rows[second])
    mixed = jnp.where(chosen, noise + signal, noise)
    return jnp.clip(mixed * row_scale, -2000.0, 2000.0).astype(jnp.bfloat16)


def with_ends(drawn, stream_key, least, top_value):
    place = [jax.random.randint(jax.random.fold_in(stream_key, axis), (), 0, length) for axis, length in enumerate(drawn.shape)]
    widest = drawn.shape.index(max(drawn.shape))
    beside = place[:widest] + [(place[widest] + 1) % drawn.shape[widest]] + place[widest + 1:]
    return drawn.at[tuple(place)].set(least).at[tuple(beside)].set(top_value)


def setup_inputs(seed: int = 0) -> dict:
    streams_of = jax.random.split(jax.random.key(seed), 7)
    drafter_hidden = draw_drafter_hidden(jax.random.fold_in(streams_of[6], 71), 0)
    norm_gain = jnp.clip(1.0 + 0.1 * jax.random.normal(streams_of[1], (D,), jnp.float32), 0.5, 1.5).astype(jnp.bfloat16)
    head_weight = draw_head_weight(jax.random.fold_in(streams_of[6], 71), 0)
    labels = with_ends(jax.random.randint(streams_of[3], (TOKENS,), 0, VOCAB), jax.random.fold_in(streams_of[3], 1), 0, VOCAB - 1).astype(jnp.int32)
    loss_mask = with_ends((jax.random.randint(streams_of[4], (TOKENS,), 0, 4) < 3).astype(jnp.int32), jax.random.fold_in(streams_of[4], 1), 0, 1)
    offsets = jax.random.randint(streams_of[5], (STEPS,), 1, MAXOFF + 1).astype(jnp.int32)
    return dict(drafter_hidden=drafter_hidden, norm_gain=norm_gain, head_weight=head_weight, labels=labels, loss_mask=loss_mask, offsets=offsets)


epsilon = 1e-05
step_decay = 0.8

def reference(drafter_hidden, norm_gain, head_weight, labels, loss_mask, offsets):
    hidden_wide = drafter_hidden.astype(jnp.float32)
    inverse = lax.rsqrt(lax.optimization_barrier(jnp.mean(hidden_wide * hidden_wide, axis=-1, keepdims=True)) + epsilon)
    normed = (hidden_wide * inverse * norm_gain.astype(jnp.float32)).astype(jnp.bfloat16)
    weight_wide = head_weight.astype(jnp.float32)
    positions = jnp.arange(TOKENS, dtype=jnp.int32)
    columns = jnp.arange(VOCAB, dtype=jnp.int32)
    block_rows = min(512, TOKENS)
    gradient = jnp.zeros((D, VOCAB), jnp.float32)
    loss_total = jnp.zeros((), jnp.float32)
    for step_at in range(STEPS):
        factor = step_decay ** step_at
        inside = positions % WINDOW + offsets[step_at] < WINDOW
        clamped = jnp.minimum(positions + offsets[step_at], TOKENS - 1).astype(jnp.int32)
        row_label = labels[clamped]
        row_weight = jnp.where(inside, loss_mask[clamped], 0).astype(jnp.float32)
        counted = jnp.sum(row_weight)
        rows_step = normed[step_at]

        def one_block(state_pair, number):
            offset_row = (number * block_rows).astype(jnp.int32)
            row_block = lax.dynamic_slice_in_dim(rows_step, offset_row, block_rows, 0)
            block_label = lax.dynamic_slice_in_dim(row_label, offset_row, block_rows, 0)
            block_weight = lax.dynamic_slice_in_dim(row_weight, offset_row, block_rows, 0)
            rows_wide = row_block.astype(jnp.float32)
            logits = jnp.dot(rows_wide, weight_wide, precision=lax.Precision.HIGHEST)
            row_top = lax.optimization_barrier(jnp.max(logits, axis=-1))
            total_exp = lax.optimization_barrier(jnp.sum(jnp.exp(logits - row_top[:, None]), axis=-1))
            log_total = row_top + jnp.log(total_exp)
            hitting = columns[None, :] == block_label[:, None]
            label_logit = lax.optimization_barrier(jnp.sum(jnp.where(hitting, logits, 0.0), axis=-1))
            numerator = jnp.sum(block_weight * (log_total - label_logit))
            softmax = jnp.exp(logits - log_total[:, None])
            slopes = (factor * block_weight[:, None] * (softmax - hitting.astype(jnp.float32))).astype(jnp.bfloat16)
            update = jnp.dot(rows_wide.T, slopes.astype(jnp.float32), precision=lax.Precision.HIGHEST)
            return ((state_pair[0] + update, state_pair[1] + numerator), None)
        start_pair = (gradient, jnp.zeros((), jnp.float32))
        finished, ignored = lax.scan(one_block, start_pair, jnp.arange(TOKENS // block_rows, dtype=jnp.int32))
        gradient = finished[0]
        loss_total = loss_total + factor * finished[1] / counted
    return (loss_total, gradient)
```

```python
import functools

import jax
import jax.numpy as jnp
from jax import lax
from jax.experimental import pallas as pl
from jax.experimental.pallas import tpu as pltpu
from jax.sharding import PartitionSpec as P

WINDOW = 512
MAXOFF = 4
LANES = 128

epsilon = 1e-05
step_decay = 0.8
MESH = pl.DeviceIdType.MESH

PACE = 2
LAG = 1
EARLY = 3


def rows_to_columns(row):
    return jnp.transpose(jnp.broadcast_to(row, (LANES, row.shape[1])))


def head_kernel(
    n, ways, x_in, gain, w_in, labels, mask, offsets, grad, loss,
    xv, held, wall, logits, s_own, s_got, labcol, wcol, lcol, tok, statall, lserow, labpart, num,
    count, sqall, invcol, lossall,
    send, recv, xsend, wsend, wrecv, sqsend, sqrecv, ssend, srecv, tsend, trecv, gsend, grecv,
    lsend, lrecv, local_sem,
):
    steps, rows, width = xv.shape
    vocab = w_in.shape[1]
    pieces = held.shape[0]
    each = rows // ways
    line = n // 4
    total_rows = n * each
    groups = total_rows // LANES
    main = steps * ways
    per_step = PACE * ways
    me, rank = lax.axis_index("dp"), lax.axis_index("tensor")
    c, x, z = lax.rem(me, 2), lax.rem(me // 2, 2), me // 4
    sibling, other = 1 - c, 1 - x
    f32 = jnp.float32

    def at(z_, x_, c_):
        return (z_ * 2 + x_) * 2 + c_

    def second(q, far):
        return main + q * (ways - 1) + far - 1

    x_load = pltpu.make_async_copy(x_in, xv, local_sem.at[0])
    x_load.start()
    w_load = pltpu.make_async_copy(w_in, wall.at[0], local_sem.at[1])
    w_load.start()

    barrier = pltpu.get_barrier_semaphore()
    for j in range(1, n):
        pl.semaphore_signal(
            barrier, inc=1, device_id={"dp": lax.rem(me + j, n)}, device_id_type=MESH
        )
    for j in range(1, ways):
        pl.semaphore_signal(
            barrier, inc=1, device_id={"tensor": lax.rem(rank + j, ways)}, device_id_type=MESH
        )

    def to_tensor(src, dst, send_sem, recv_sem, far):
        return pltpu.make_async_remote_copy(
            src_ref=src,
            dst_ref=dst,
            send_sem=send_sem,
            recv_sem=recv_sem,
            device_id={"tensor": lax.rem(rank + far, ways)},
            device_id_type=MESH,
        )

    def to_dp(src, dst, send_sem, recv_sem, target):
        return pltpu.make_async_remote_copy(
            src_ref=src,
            dst_ref=dst,
            send_sem=send_sem,
            recv_sem=recv_sem,
            device_id={"dp": target},
            device_id_type=MESH,
        )

    def square_copy(far):
        return to_tensor(
            sqall.at[0], sqall.at[ways - far], sqsend.at[far - 1], sqrecv.at[ways - far - 1], far
        )

    def w_copy(far):
        return to_tensor(
            w_in, wall.at[ways - far], wsend.at[far - 1], wrecv.at[ways - far - 1], far
        )

    def x_copy(q, far):
        target = q * ways + ways - far
        return to_tensor(
            held.at[second(q, far), me],
            held.at[target, me],
            xsend.at[q, far - 1],
            recv.at[target, me],
            far,
        )

    def slope_copy(q, far):
        return to_tensor(
            s_own.at[q],
            s_got.at[ways - far - 1, q],
            gsend.at[far - 1, q],
            grecv.at[ways - far - 1, q],
            far,
        )

    def loss_copy(far):
        return to_tensor(
            lossall.at[0], lossall.at[ways - far], lsend.at[far - 1], lrecv.at[ways - far - 1], far
        )

    def token_copy(j):
        target = lax.rem(me + j, n)
        return to_dp(tok.at[me], tok.at[me], tsend.at[j], trecv.at[me], target)

    def token_wait(j):
        source = lax.rem(me + j, n)
        return to_dp(tok.at[source], tok.at[source], tsend.at[j], trecv.at[source], source)

    def stat_copy(q, j):
        target = lax.rem(me + j, n)
        return to_dp(
            statall.at[q, me], statall.at[q, me], ssend.at[q, j], srecv.at[q, me], target
        )

    def stat_wait(q, j):
        source = lax.rem(me + j, n)
        return to_dp(
            statall.at[q, source], statall.at[q, source], ssend.at[q, j], srecv.at[q, source], source
        )

    def block_copy(kind, i, b, target):
        return to_dp(held.at[i, b], held.at[i, b], send.at[kind, i, b // 2], recv.at[i, b], target)

    def ups(i, b):
        return block_copy(0, i, b, at(z + 1, x, c))

    def downs(i, b):
        return block_copy(1, i, b, at(z - 1, x, c))

    def across(i, b):
        return block_copy(2, i, b, at(z, other, c))

    def beside(i, b):
        return block_copy(3, i, b, at(z, x, sibling))

    def inside(zz):
        return jnp.logical_and(zz >= 0, zz < line)

    top_half = lax.broadcasted_iota(jnp.int32, (8, rows), 0) < 4
    tok[me] = jnp.where(
        top_half,
        jnp.broadcast_to(labels[...], (8, rows)),
        jnp.broadcast_to(mask[...], (8, rows)),
    )
    x_load.wait()
    for s in range(steps):

        def square(j, acc):
            part = xv[s, :, pl.ds(pl.multiple_of(j * LANES, LANES), LANES)].astype(f32)
            return acc + part * part

        acc = lax.fori_loop(0, width // LANES, square, jnp.zeros((rows, LANES), f32))
        column = jnp.sum(acc, axis=1, keepdims=True)
        flat = jnp.transpose(jnp.broadcast_to(column, (rows, LANES)))
        sqall[0, s] = flat[0:8]

    peers = n - 1 + ways - 1
    pl.semaphore_wait(barrier, peers)
    for far in range(1, ways):
        square_copy(far).start()
    for j in range(1, n):
        token_copy(j).start()
    labpart[...] = jnp.zeros_like(labpart)
    num[...] = jnp.zeros_like(num)
    count[...] = jnp.zeros_like(count)
    statall[:, me] = jnp.zeros((steps, 2, 8, LANES), f32)
    for far in range(1, ways):
        square_copy(far).wait_recv()
    for s in range(steps):
        total = sqall[0, s]
        for p in range(1, ways):
            total = total + sqall[p, s]
        inverse = lax.rsqrt(total / (width * ways) + epsilon)
        invcol[s] = rows_to_columns(inverse[0:1])

    for s in range(steps):
        for far in range(ways):
            owner = lax.rem(rank + far, ways)
            offset = pl.multiple_of(owner * each, each)
            i = second(s, far) if far else s * ways
            scale = invcol[s, pl.ds(offset, each)]

            def normalise(j, carry, s=s, i=i, offset=offset, scale=scale):
                at_lane = pl.ds(pl.multiple_of(j * LANES, LANES), LANES)
                wide = xv[s, pl.ds(offset, each), at_lane].astype(f32)
                held[i, me, :, at_lane] = (wide * scale * gain[:, at_lane].astype(f32)).astype(
                    jnp.bfloat16
                )
                return carry

            lax.fori_loop(0, width // LANES, normalise, 0)
    for s in range(steps):
        for far in range(1, ways):
            x_copy(s, far).start()
    for far in range(1, ways):
        w_copy(far).start()

    def relay(i, k):
        valid = jnp.logical_and(jnp.logical_and(i >= 0, i < pieces), k <= line)
        early = lax.rem(i, 6) == EARLY
        foreign = jnp.logical_and(i < main, lax.rem(i, ways) > 0)

        def along(zz, b):
            @pl.when(jnp.logical_and(zz <= z, z < line - 1))
            def _():
                ups(i, b).start()

            @pl.when(jnp.logical_and(zz >= z, z > 0))
            def _():
                downs(i, b).start()

        for side in (0, 1):
            zz = z + k if side else z - k
            ok = jnp.logical_and(inside(zz), k >= side)

            @pl.when(jnp.logical_and(valid, ok))
            def _(zz=zz):
                b = at(zz, x, c)

                @pl.when(jnp.logical_or(k > 0, foreign))
                def _():
                    beside(i, b).wait_recv()

                along(zz, b)

                @pl.when(jnp.logical_or(k == 0, jnp.logical_not(early)))
                def _():
                    across(i, b).start()

                beside(i, b).start()

        for side in (0, 1):
            zz = z + (k - 1) if side else z - (k - 1)
            ok = jnp.logical_and(inside(zz), k > side)

            @pl.when(jnp.logical_and(valid, ok))
            def _(zz=zz):
                b = at(zz, other, c)
                beside(i, b).wait_recv()

                @pl.when(early)
                def _():
                    along(zz, b)

                beside(i, b).start()

    def token_block(b):
        here = tok[b].astype(f32)
        following = tok[jnp.minimum(b + 1, n - 1)].astype(f32)
        last = jnp.broadcast_to(here[:, rows - 1 : rows], (8, rows))
        following = jnp.where(b == n - 1, last, following)
        lane = lax.broadcasted_iota(jnp.int32, (8, rows), 1)
        position = lax.rem(b * rows + lane, WINDOW)
        for s in range(steps):
            by = offsets[s]
            chosen = here
            for far in range(1, MAXOFF + 1):
                shifted = jnp.where(
                    lane < rows - far,
                    pltpu.roll(here, rows - far, 1),
                    pltpu.roll(following, rows - far, 1),
                )
                chosen = jnp.where(by == far, shifted, chosen)
            weight = jnp.where(position + by < WINDOW, chosen, 0.0)[4:5]
            count[s, 0:1] = count[s, 0:1] + weight
            span = pl.ds(pl.multiple_of(b * rows, rows), rows)
            labcol[s, span] = rows_to_columns(chosen[0:1])
            wcol[s, span] = rows_to_columns(weight)

    def own_span(b):
        return pl.ds(pl.multiple_of(b * rows + rank * each, each), each)

    def hits(s, b, chunk):
        columns = (
            me * vocab + chunk * LANES + lax.broadcasted_iota(jnp.int32, (each, LANES), 1)
        ).astype(f32)
        return labcol[s, own_span(b)] == columns

    def folded(values):
        return jnp.sum(values.reshape(each // 8, 8, LANES), axis=0)

    def logits_unit(q, zz):
        for core_x in range(2):
            for p in range(ways):
                b = at(zz, core_x, sibling)
                beside(q * ways + p, b).wait_recv()
        acc = None
        for p in range(ways):
            lhs = held[q * ways + p, pl.ds(4 * zz, 4)].reshape(4 * each, width)
            part = jnp.dot(lhs, wall[p], preferred_element_type=f32)
            acc = part if acc is None else acc + part
        span = pl.ds(pl.multiple_of(zz * 4 * each, 4 * each), 4 * each)
        logits[q, span] = acc

        def block_stats(j, carry):
            b = 4 * zz + j
            span = pl.ds(pl.multiple_of(b * each, each), each)
            tile = logits[q, span]
            top = jnp.max(tile, axis=1, keepdims=True)
            lse = top + jnp.log(jnp.sum(jnp.exp(tile - top), axis=1, keepdims=True))
            lcol[q, span] = jnp.broadcast_to(lse, (each, LANES))
            found = jnp.zeros((each, LANES), f32)
            for chunk in range(vocab // LANES):
                part = tile[:, chunk * LANES : (chunk + 1) * LANES]
                found = found + jnp.where(hits(q, b, chunk), part, 0.0)
            labpart[q] = labpart[q] + folded(wcol[q, own_span(b)] * found)
            return carry

        lax.fori_loop(0, 4, block_stats, 0)

    def send_stats(q):
        def group(g, carry):
            tile = lcol[q, pl.ds(pl.multiple_of(g * LANES, LANES), LANES)]
            statall[q, me, 0, pl.ds(g, 1)] = jnp.transpose(tile)[0:1]
            return carry

        lax.fori_loop(0, groups, group, 0)
        statall[q, me, 1] = labpart[q]
        for j in range(1, n):
            stat_copy(q, j).start()

    def make_slopes(q):
        for j in range(1, n):
            stat_wait(q, j).wait_recv()

        def highest(j, top):
            return jnp.maximum(top, statall[q, j, 0])

        top = lax.fori_loop(1, n, highest, statall[q, 0, 0])

        def sums(j, carry):
            total, found = carry
            return total + jnp.exp(statall[q, j, 0] - top), found + statall[q, j, 1]

        zero = jnp.zeros((8, LANES), f32)
        total, found = lax.fori_loop(0, n, sums, (zero, zero))
        lserow[q] = top + jnp.log(total)

        def group(g, carry):
            span = pl.ds(pl.multiple_of(g * LANES, LANES), LANES)
            lcol[q, span] = rows_to_columns(lserow[q, pl.ds(g, 1)])
            return carry

        lax.fori_loop(0, groups, group, 0)
        factor = jnp.float32(1.0)
        for s in range(1, steps):
            factor = jnp.where(q == s, jnp.float32(step_decay**s), factor)

        def block(b, carry):
            span = pl.ds(pl.multiple_of(b * each, each), each)
            lse = lcol[q, span]
            weight = wcol[q, own_span(b)]
            scale = factor * weight
            for chunk in range(vocab // LANES):
                lanes = pl.ds(chunk * LANES, LANES)
                softmax = jnp.exp(logits[q, span, lanes] - lse)
                hit = jnp.where(hits(q, b, chunk), 1.0, 0.0)
                s_own[q, span, lanes] = (scale * (softmax - hit)).astype(jnp.bfloat16)
            return carry + folded(weight * lse)

        weighted = lax.fori_loop(0, n, block, zero)
        for far in range(1, ways):
            slope_copy(q, far).start()
        numerator = jnp.sum(weighted, axis=0, keepdims=True) - jnp.sum(
            jnp.sum(found, axis=0, keepdims=True), axis=1, keepdims=True
        )
        num[q] = jnp.broadcast_to(numerator, (8, LANES))

    def add_gradient(i, slopes, first):
        block = 256 if width % 256 == 0 else LANES

        def part(j, carry):
            lanes = pl.ds(pl.multiple_of(j * block, block), block)
            lhs = held[i, :, :, lanes].reshape(total_rows, block)
            value = lax.dot_general(
                lhs, slopes[...], (((0,), (0,)), ((), ())), preferred_element_type=f32
            )

            @pl.when(first)
            def _():
                grad[lanes, :] = value

            @pl.when(jnp.logical_not(first))
            def _():
                grad[lanes, :] = grad[lanes, :] + value

            return carry

        lax.fori_loop(0, width // block, part, 0)

    base = PACE * (ways - 1) + 2
    slopes_base = base + line - 1 + LAG
    got_base = PACE * (main + ways - 2) + line + 1
    got_pace = PACE * (ways - 1)
    depth = line // PACE + 1

    def wave(w, carry):
        for d in range(depth - 1, -1, -1):
            i = w // PACE - d
            relay(i, w - PACE * i)

        @pl.when(jnp.logical_and(w >= 1, w <= line))
        def _():
            @pl.when(w == 1)
            def _():
                for j in range(1, n):
                    token_wait(j).wait_recv()

            def one(j, carry):
                token_block(4 * (w - 1) + j)
                return carry

            lax.fori_loop(0, 4, one, 0)

        @pl.when(w == base)
        def _():
            w_load.wait()
            for far in range(1, ways):
                w_copy(far).wait_recv()

        t = w - base
        q, u = t // per_step, lax.rem(t, per_step)
        active = jnp.logical_and(t >= 0, jnp.logical_and(q < steps, u < line))

        @pl.when(active)
        def _():
            def one(side, carry):
                zz = z + u * (2 * side - 1)

                @pl.when(jnp.logical_and(inside(zz), u >= side))
                def _():
                    logits_unit(q, zz)

                return carry

            lax.fori_loop(0, 2, one, 0)

            @pl.when(u == line - 1)
            def _():
                send_stats(q)

        ts = w - slopes_base
        qs = ts // per_step

        @pl.when(jnp.logical_and(jnp.logical_and(ts >= 0, lax.rem(ts, per_step) == 0), qs < steps))
        def _():
            make_slopes(qs)

            @pl.when(qs == steps - 1)
            def _():
                lossall[0] = num[...]
                for far in range(1, ways):
                    loss_copy(far).start()

            add_gradient(qs * ways, s_own.at[qs], qs == 0)

        tg = w - got_base
        qg = tg // got_pace

        @pl.when(jnp.logical_and(jnp.logical_and(tg >= 0, lax.rem(tg, got_pace) == 0), qg < steps))
        def _():
            for far in range(1, ways):
                i = second(qg, far)
                slope_copy(qg, ways - far).wait_recv()

                def arrived(j, carry, i=i):
                    beside(i, 2 * j + sibling).wait_recv()
                    return carry

                lax.fori_loop(0, 2 * line, arrived, 0)
                add_gradient(i, s_got.at[far - 1, qg], False)

        return carry

    waves = max(
        PACE * (pieces - 1) + line + 1,
        slopes_base + (steps - 1) * per_step + 1,
        got_base + (steps - 1) * got_pace + 1,
    )
    lax.fori_loop(0, waves, wave, 0)

    for far in range(1, ways):
        loss_copy(far).wait_recv()
    result = jnp.zeros((8, LANES), f32)
    for s in range(steps):
        numerator = lossall[0, s]
        for p in range(1, ways):
            numerator = numerator + lossall[p, s]
        counted = jnp.sum(
            jnp.sum(count[s], axis=0, keepdims=True), axis=1, keepdims=True
        )
        result = result + step_decay**s * numerator / jnp.broadcast_to(counted, (8, LANES))
    loss[...] = result

    def finish(u, carry):
        i, b = u // n, lax.rem(u, n)
        early = lax.rem(i, 6) == EARLY
        cb, xb, zb = lax.rem(b, 2), lax.rem(b // 2, 2), b // 4
        mine = cb == c
        column = jnp.logical_and(mine, xb == x)
        lined = jnp.logical_and(mine, jnp.logical_or(xb == x, early))

        @pl.when(jnp.logical_and(lined, jnp.logical_and(zb <= z, z < line - 1)))
        def _():
            ups(i, b).wait_send()

        @pl.when(jnp.logical_and(lined, jnp.logical_and(zb >= z, z > 0)))
        def _():
            downs(i, b).wait_send()

        @pl.when(jnp.logical_and(column, jnp.logical_or(zb == z, jnp.logical_not(early))))
        def _():
            across(i, b).wait_send()

        @pl.when(mine)
        def _():
            beside(i, b).wait_send()

        return carry

    lax.fori_loop(0, pieces * n, finish, 0)
    for j in range(1, n):
        token_copy(j).wait_send()
    for far in range(1, ways):
        square_copy(far).wait_send()
        w_copy(far).wait_send()
        loss_copy(far).wait_send()
    for s in range(steps):
        for j in range(1, n):
            stat_copy(s, j).wait_send()
        for far in range(1, ways):
            x_copy(s, far).wait_send()
            slope_copy(s, far).wait_send()


def head_step(hidden, gain, weight, labels, mask, offsets):
    steps, rows, width = hidden.shape
    vocab = weight.shape[1]
    n, ways = lax.axis_size("dp"), lax.axis_size("tensor")
    each = rows // ways
    total_rows = n * each
    pieces = steps * (2 * ways - 1)
    vmem = pl.BlockSpec(memory_space=pltpu.VMEM)
    smem = pl.BlockSpec(memory_space=pltpu.SMEM)
    hbm = pl.BlockSpec(memory_space=pl.ANY)
    dma = pltpu.SemaphoreType.DMA
    f32, bf16 = jnp.float32, jnp.bfloat16
    return pl.pallas_call(
        functools.partial(head_kernel, n, ways),
        out_shape=[
            jax.ShapeDtypeStruct((width, vocab), f32),
            jax.ShapeDtypeStruct((8, LANES), f32),
        ],
        in_specs=[hbm, vmem, hbm, vmem, vmem, smem],
        out_specs=[vmem, vmem],
        scratch_shapes=[
            pltpu.VMEM((steps, rows, width), bf16),
            pltpu.VMEM((pieces, n, each, width), bf16),
            pltpu.VMEM((ways, width, vocab), bf16),
            pltpu.VMEM((steps, total_rows, vocab), f32),
            pltpu.VMEM((steps, total_rows, vocab), bf16),
            pltpu.VMEM((ways - 1, steps, total_rows, vocab), bf16),
            pltpu.VMEM((steps, n * rows, LANES), f32),
            pltpu.VMEM((steps, n * rows, LANES), f32),
            pltpu.VMEM((steps, total_rows, LANES), f32),
            pltpu.VMEM((n, 8, rows), jnp.int32),
            pltpu.VMEM((steps, n, 2, 8, LANES), f32),
            pltpu.VMEM((steps, 8, LANES), f32),
            pltpu.VMEM((steps, 8, LANES), f32),
            pltpu.VMEM((steps, 8, LANES), f32),
            pltpu.VMEM((steps, 8, rows), f32),
            pltpu.VMEM((ways, steps, 8, rows), f32),
            pltpu.VMEM((steps, rows, LANES), f32),
            pltpu.VMEM((ways, steps, 8, LANES), f32),
            dma((4, pieces, n // 2)),
            dma((pieces, n)),
            dma((steps, ways - 1)),
            dma((ways - 1,)),
            dma((ways - 1,)),
            dma((ways - 1,)),
            dma((ways - 1,)),
            dma((steps, n)),
            dma((steps, n)),
            dma((n,)),
            dma((n,)),
            dma((ways - 1, steps)),
            dma((ways - 1, steps)),
            dma((ways - 1,)),
            dma((ways - 1,)),
            dma((2,)),
        ],
        compiler_params=pltpu.CompilerParams(
            collective_id=7, has_side_effects=True, vmem_limit_bytes=60 * 1024 * 1024
        ),
        name="head_step",
    )(hidden, gain, weight, labels, mask, offsets)


def local(drafter_hidden, norm_gain, head_weight, labels, loss_mask, offsets):
    gradient, loss = head_step(
        drafter_hidden, norm_gain[None], head_weight, labels[None], loss_mask[None], offsets
    )
    return (loss[0, 0], gradient)


def solution(mesh):
    return jax.shard_map(
        local,
        mesh=mesh,
        in_specs=(P(None, "dp", "tensor"), P("tensor"), P("tensor", "dp"), P("dp"), P("dp"), P()),
        out_specs=(P(), P("tensor", "dp")),
        check_vma=False,
    )
```

```python
import functools

import jax
import jax.numpy as jnp
from jax import lax
from jax.experimental import pallas as pl
from jax.experimental.pallas import tpu as pltpu
from jax.sharding import PartitionSpec as P

WINDOW = 512
MAXOFF = 4
LANES = 128

epsilon = 1e-05
step_decay = 0.8
MESH = pl.DeviceIdType.MESH

SPLIT = 2
GAP = 3
SPACE = 3
UNIT = 1
LAG = 3
OWN = 6
EARLY = 1
HOLD = 18


def rows_to_columns(row):
    return jnp.transpose(jnp.broadcast_to(row, (LANES, row.shape[1])))


def head_kernel(
    n, ways, x_in, gain, w_in, labels, mask, offsets, grad_out, loss,
    grad, xv, held, wall, logits, s_own, s_got, labcol, wcol, lcol, tok, statall, lserow, labpart, num,
    count, sqall, invcol, lossall,
    send, recv, xsend, wsend, wrecv, sqsend, sqrecv, ssend, srecv, tsend, trecv, gsend, grecv,
    lsend, lrecv, local_sem, out_sem,
):
    steps, rows, width = xv.shape
    vocab = w_in.shape[1]
    pieces, few = held.shape[0], held.shape[2]
    each = rows // ways
    split = each // few
    chunks = steps * split
    line = n // 4
    chunk_rows = n * few
    groups = chunk_rows // LANES
    main = chunks * ways
    me, rank = lax.axis_index("dp"), lax.axis_index("tensor")
    c, x, z = lax.rem(me, 2), lax.rem(me // 2, 2), me // 4
    sibling, other = 1 - c, 1 - x
    f32 = jnp.float32

    def at(z_, x_, c_):
        return (z_ * 2 + x_) * 2 + c_

    def first(q, p):
        return q * ways + p

    def second(q, far):
        return main + q * (ways - 1) + far - 1

    x_load = pltpu.make_async_copy(x_in, xv, local_sem.at[0])
    x_load.start()
    w_load = pltpu.make_async_copy(w_in, wall.at[0], local_sem.at[1])
    w_load.start()

    barrier = pltpu.get_barrier_semaphore()
    for j in range(1, n):
        pl.semaphore_signal(
            barrier, inc=1, device_id={"dp": lax.rem(me + j, n)}, device_id_type=MESH
        )
    for j in range(1, ways):
        pl.semaphore_signal(
            barrier, inc=1, device_id={"tensor": lax.rem(rank + j, ways)}, device_id_type=MESH
        )

    def to_tensor(src, dst, send_sem, recv_sem, far):
        return pltpu.make_async_remote_copy(
            src_ref=src,
            dst_ref=dst,
            send_sem=send_sem,
            recv_sem=recv_sem,
            device_id={"tensor": lax.rem(rank + far, ways)},
            device_id_type=MESH,
        )

    def to_dp(src, dst, send_sem, recv_sem, target):
        return pltpu.make_async_remote_copy(
            src_ref=src,
            dst_ref=dst,
            send_sem=send_sem,
            recv_sem=recv_sem,
            device_id={"dp": target},
            device_id_type=MESH,
        )

    def square_copy(far):
        return to_tensor(
            sqall.at[0], sqall.at[ways - far], sqsend.at[far - 1], sqrecv.at[ways - far - 1], far
        )

    def w_copy(far):
        return to_tensor(
            w_in, wall.at[ways - far], wsend.at[far - 1], wrecv.at[ways - far - 1], far
        )

    def x_copy(q, far):
        target = first(q, ways - far)
        return to_tensor(
            held.at[second(q, far), me],
            held.at[target, me],
            xsend.at[q, far - 1],
            recv.at[target, me],
            far,
        )

    def slope_copy(q, far):
        return to_tensor(
            s_own.at[q],
            s_got.at[ways - far - 1, q],
            gsend.at[far - 1, q],
            grecv.at[ways - far - 1, q],
            far,
        )

    def loss_copy(far):
        return to_tensor(
            lossall.at[0], lossall.at[ways - far], lsend.at[far - 1], lrecv.at[ways - far - 1], far
        )

    def token_copy(j):
        target = lax.rem(me + j, n)
        return to_dp(tok.at[me], tok.at[me], tsend.at[j], trecv.at[me], target)

    def token_wait(j):
        source = lax.rem(me + j, n)
        return to_dp(tok.at[source], tok.at[source], tsend.at[j], trecv.at[source], source)

    def stat_copy(q, j):
        target = lax.rem(me + j, n)
        return to_dp(
            statall.at[q, me], statall.at[q, me], ssend.at[q, j], srecv.at[q, me], target
        )

    def stat_wait(q, j):
        source = lax.rem(me + j, n)
        return to_dp(
            statall.at[q, source], statall.at[q, source], ssend.at[q, j], srecv.at[q, source], source
        )

    def block_copy(kind, i, b, target):
        return to_dp(held.at[i, b], held.at[i, b], send.at[kind, i, b // 2], recv.at[i, b], target)

    def ups(i, b):
        return block_copy(0, i, b, at(z + 1, x, c))

    def downs(i, b):
        return block_copy(1, i, b, at(z - 1, x, c))

    def across(i, b):
        return block_copy(2, i, b, at(z, other, c))

    def beside(i, b):
        return block_copy(3, i, b, at(z, x, sibling))

    def inside(zz):
        return jnp.logical_and(zz >= 0, zz < line)

    top_half = lax.broadcasted_iota(jnp.int32, (8, rows), 0) < 4
    tok[me] = jnp.where(
        top_half,
        jnp.broadcast_to(labels[...], (8, rows)),
        jnp.broadcast_to(mask[...], (8, rows)),
    )
    x_load.wait()
    for s in range(steps):

        def square(j, acc):
            part = xv[s, :, pl.ds(pl.multiple_of(j * LANES, LANES), LANES)].astype(f32)
            return acc + part * part

        acc = lax.fori_loop(0, width // LANES, square, jnp.zeros((rows, LANES), f32))
        column = jnp.sum(acc, axis=1, keepdims=True)
        flat = jnp.transpose(jnp.broadcast_to(column, (rows, LANES)))
        sqall[0, s] = flat[0:8]

    peers = n - 1 + ways - 1
    pl.semaphore_wait(barrier, peers)
    for far in range(1, ways):
        square_copy(far).start()
    for j in range(1, n):
        token_copy(j).start()
    labpart[...] = jnp.zeros_like(labpart)
    num[...] = jnp.zeros_like(num)
    count[...] = jnp.zeros_like(count)
    statall[:, me] = jnp.zeros((chunks, 2, 8, LANES), f32)
    for far in range(1, ways):
        square_copy(far).wait_recv()
    for s in range(steps):
        total = sqall[0, s]
        for p in range(1, ways):
            total = total + sqall[p, s]
        inverse = lax.rsqrt(total / (width * ways) + epsilon)
        invcol[s] = rows_to_columns(inverse[0:1])

    for s in range(steps):
        for far in range(ways):
            owner = lax.rem(rank + far, ways)
            offset = pl.multiple_of(owner * each, each)
            scale = jnp.concatenate([invcol[s, pl.ds(offset, each)]] * 2, axis=1)

            def normalise(j, carry, s=s, far=far, offset=offset, scale=scale):
                at_lane = pl.ds(pl.multiple_of(j * 2 * LANES, 2 * LANES), 2 * LANES)
                wide = xv[s, pl.ds(offset, each), at_lane].astype(f32)
                value = (wide * scale * gain[at_lane].astype(f32)[None]).astype(jnp.bfloat16)
                for sub in range(split):
                    q = s * split + sub
                    i = second(q, far) if far else first(q, 0)
                    held[i, me, :, at_lane] = value[sub * few : (sub + 1) * few]
                return carry

            lax.fori_loop(0, width // (2 * LANES), normalise, 0)
    for q in range(chunks):
        for far in range(1, ways):
            x_copy(q, far).start()
    for far in range(1, ways):
        w_copy(far).start()

    def relay(k, t):
        j = lax.rem(t, GAP * ways)
        i = ways * (t // (GAP * ways)) + j
        valid = jnp.logical_and(jnp.logical_and(t >= 0, j < ways), i < pieces)
        early = lax.rem(i, 6) == EARLY
        foreign = jnp.logical_and(i < main, lax.rem(i, ways) > 0)

        def along(zz, b):
            @pl.when(jnp.logical_and(zz <= z, z < line - 1))
            def _():
                ups(i, b).start()

            @pl.when(jnp.logical_and(zz >= z, z > 0))
            def _():
                downs(i, b).start()

        for side in (0, 1):
            zz = z + k if side else z - k
            ok = jnp.logical_and(inside(zz), k >= side)

            @pl.when(jnp.logical_and(valid, ok))
            def _(zz=zz):
                b = at(zz, x, c)

                @pl.when(jnp.logical_or(k > 0, foreign))
                def _():
                    beside(i, b).wait_recv()

                along(zz, b)

                @pl.when(jnp.logical_or(k == 0, jnp.logical_not(early)))
                def _():
                    across(i, b).start()

                beside(i, b).start()

        for side in (0, 1):
            zz = z + (k - 1) if side else z - (k - 1)
            ok = jnp.logical_and(inside(zz), k > side)

            @pl.when(jnp.logical_and(valid, ok))
            def _(zz=zz):
                b = at(zz, other, c)
                beside(i, b).wait_recv()

                @pl.when(early)
                def _():
                    along(zz, b)

                beside(i, b).start()

    def drain(i, carry):
        early = lax.rem(i, 6) == EARLY

        def one(zz, carry):
            own, far_side = at(zz, x, c), at(zz, other, c)
            up = jnp.logical_and(zz <= z, z < line - 1)
            down = jnp.logical_and(zz >= z, z > 0)
            beside(i, own).wait_send()
            beside(i, far_side).wait_send()

            @pl.when(up)
            def _():
                ups(i, own).wait_send()

            @pl.when(down)
            def _():
                downs(i, own).wait_send()

            @pl.when(jnp.logical_or(zz == z, jnp.logical_not(early)))
            def _():
                across(i, own).wait_send()

            @pl.when(early)
            def _():
                @pl.when(up)
                def _():
                    ups(i, far_side).wait_send()

                @pl.when(down)
                def _():
                    downs(i, far_side).wait_send()

            return carry

        lax.fori_loop(0, line, one, 0)
        return carry

    def token_block(b):
        here = tok[b].astype(f32)
        following = tok[jnp.minimum(b + 1, n - 1)].astype(f32)
        last = jnp.broadcast_to(here[:, rows - 1 : rows], (8, rows))
        following = jnp.where(b == n - 1, last, following)
        lane = lax.broadcasted_iota(jnp.int32, (8, rows), 1)
        position = lax.rem(b * rows + lane, WINDOW)
        for s in range(steps):
            by = offsets[s]
            chosen = here
            for far in range(1, MAXOFF + 1):
                shifted = jnp.where(
                    lane < rows - far,
                    pltpu.roll(here, rows - far, 1),
                    pltpu.roll(following, rows - far, 1),
                )
                chosen = jnp.where(by == far, shifted, chosen)
            weight = jnp.where(position + by < WINDOW, chosen, 0.0)[4:5]
            count[s, 0:1] = count[s, 0:1] + weight
            span = pl.ds(pl.multiple_of(b * rows, rows), rows)
            labcol[s, span] = rows_to_columns(chosen[0:1])
            wcol[s, span] = rows_to_columns(weight)

    def tokens(q, b):
        start = b * rows + rank * each + lax.rem(q, split) * few
        return q // split, pl.ds(pl.multiple_of(start, few), few)

    def hits(q, b, chunk):
        columns = (
            me * vocab + chunk * LANES + lax.broadcasted_iota(jnp.int32, (few, LANES), 1)
        ).astype(f32)
        return labcol[tokens(q, b)] == columns

    def folded(values):
        return jnp.sum(values.reshape(few // 8, 8, LANES), axis=0)

    def logits_unit(q, zz):
        acc = None
        for p in range(ways):
            for core_x in range(2):
                beside(first(q, p), at(zz, core_x, sibling)).wait_recv()
        for p in range(ways):
            lhs = held[first(q, p), pl.ds(4 * zz, 4)].reshape(4 * few, width)
            part = jnp.dot(lhs, wall[p], preferred_element_type=f32)
            acc = part if acc is None else acc + part
        logits[q, pl.ds(4 * zz, 4)] = acc.reshape(4, few, vocab)

        def block_stats(j, carry):
            b = 4 * zz + j
            span = pl.ds(pl.multiple_of(b * few, few), few)
            tile = logits[q, b]
            top = jnp.max(tile, axis=1, keepdims=True)
            lse = top + jnp.log(jnp.sum(jnp.exp(tile - top), axis=1, keepdims=True))
            lcol[q, span] = jnp.broadcast_to(lse, (few, LANES))
            found = jnp.zeros((few, LANES), f32)
            for chunk in range(vocab // LANES):
                part = tile[:, chunk * LANES : (chunk + 1) * LANES]
                found = found + jnp.where(hits(q, b, chunk), part, 0.0)
            labpart[q] = labpart[q] + folded(wcol[tokens(q, b)] * found)
            return carry

        lax.fori_loop(0, 4, block_stats, 0)

    def send_stats(q):
        def group(g, carry):
            tile = lcol[q, pl.ds(pl.multiple_of(g * LANES, LANES), LANES)]
            statall[q, me, 0, pl.ds(g, 1)] = jnp.transpose(tile)[0:1]
            return carry

        lax.fori_loop(0, groups, group, 0)
        statall[q, me, 1] = labpart[q]
        for j in range(1, n):
            stat_copy(q, j).start()

    def make_slopes(q):
        for j in range(1, n):
            stat_wait(q, j).wait_recv()

        def highest(j, top):
            return jnp.maximum(top, statall[q, j, 0])

        top = lax.fori_loop(1, n, highest, statall[q, 0, 0])

        def sums(j, carry):
            total, found = carry
            return total + jnp.exp(statall[q, j, 0] - top), found + statall[q, j, 1]

        zero = jnp.zeros((8, LANES), f32)
        total, found = lax.fori_loop(0, n, sums, (zero, zero))
        lserow[q] = top + jnp.log(total)

        def group(g, carry):
            span = pl.ds(pl.multiple_of(g * LANES, LANES), LANES)
            lcol[q, span] = rows_to_columns(lserow[q, pl.ds(g, 1)])
            return carry

        lax.fori_loop(0, groups, group, 0)
        factor = jnp.float32(1.0)
        for s in range(1, steps):
            factor = jnp.where(q // split == s, jnp.float32(step_decay**s), factor)

        def block(b, carry):
            span = pl.ds(pl.multiple_of(b * few, few), few)
            lse = lcol[q, span]
            weight = wcol[tokens(q, b)]
            scale = factor * weight
            for chunk in range(vocab // LANES):
                lanes = pl.ds(chunk * LANES, LANES)
                softmax = jnp.exp(logits[q, b, :, lanes] - lse)
                hit = jnp.where(hits(q, b, chunk), 1.0, 0.0)
                s_own[q, b, :, lanes] = (scale * (softmax - hit)).astype(jnp.bfloat16)
            return carry + folded(weight * lse)

        weighted = lax.fori_loop(0, n, block, zero)
        for far in range(1, ways):
            slope_copy(q, far).start()
        numerator = jnp.sum(weighted, axis=0, keepdims=True) - jnp.sum(
            jnp.sum(found, axis=0, keepdims=True), axis=1, keepdims=True
        )
        num[q] = jnp.broadcast_to(numerator, (8, LANES))

    block = 256 if width % 256 == 0 else LANES
    blocks = width // block

    def out_copy(j):
        lanes = pl.ds(pl.multiple_of(j * block, block), block)
        return pltpu.make_async_copy(grad.at[lanes], grad_out.at[lanes], out_sem.at[j])

    def add_gradient(i, slopes, first_time, last_time):

        def part(j, carry):
            lanes = pl.ds(pl.multiple_of(j * block, block), block)
            lhs = held[i, :, :, lanes].reshape(chunk_rows, block)
            rhs = slopes[...].reshape(chunk_rows, vocab)
            value = lax.dot_general(
                lhs, rhs, (((0,), (0,)), ((), ())), preferred_element_type=f32
            )

            @pl.when(first_time)
            def _():
                grad[lanes, :] = value

            @pl.when(jnp.logical_not(first_time))
            def _():
                grad[lanes, :] = grad[lanes, :] + value

            @pl.when(jnp.logical_and(last_time, j > 0))
            def _():
                out_copy(j - 1).start()

            return carry

        lax.fori_loop(0, blocks, part, 0)

    def larger(a, b):
        both = isinstance(a, int) and isinstance(b, int)
        return max(a, b) if both else jnp.maximum(a, b)

    def ready(i, k):
        return GAP * ways * (i // ways) + i % ways + SPACE * k

    def unit_slot(q, u):
        held_back = HOLD + q * line + u - 1000 * (q // split)
        return larger(ready(q * ways + ways - 1, u + 1) + UNIT, larger(held_back, HOLD))

    def slopes_slot(q):
        return unit_slot(q, line - 1) + LAG

    def got_slot(q):
        return larger(ready(second(q, ways - 1), line), slopes_slot(q)) + 1

    final = chunks - 1
    slots = 1 + max(ready(pieces - 1, line), slopes_slot(final) + OWN, got_slot(final))
    assert slopes_slot(0) + OWN < got_slot(0) and slopes_slot(final) + OWN < got_slot(final)
    assert all(unit_slot(q, 0) >= unit_slot(0, 0) for q in range(chunks))
    drained = sum(ready(i, line + 2) < slots for i in range(pieces))

    def slot(w, carry):
        for k in range(line, -1, -1):
            relay(k, w - SPACE * k)
        t = w - SPACE * (line + 2)
        i = ways * (t // (GAP * ways)) + lax.rem(t, GAP * ways)

        @pl.when(jnp.logical_and(t >= 0, jnp.logical_and(lax.rem(t, GAP * ways) < ways, i < drained)))
        def _():
            drain(i, 0)

        @pl.when(jnp.logical_and(w >= 1, w <= n))
        def _():
            @pl.when(w == 1)
            def _():
                for j in range(1, n):
                    token_wait(j).wait_recv()

            token_block(w - 1)

        @pl.when(w == unit_slot(0, 0))
        def _():
            w_load.wait()
            for far in range(1, ways):
                w_copy(far).wait_recv()

        def chunk(q, carry):
            @pl.when(jnp.logical_and(w >= unit_slot(q, 0), w <= unit_slot(q, line - 1)))
            def _():
                def unit(v, carry):
                    u, side = v // 2, lax.rem(v, 2)
                    zz = z + u * (2 * side - 1)
                    now = jnp.logical_and(w == unit_slot(q, u), u >= side)

                    @pl.when(jnp.logical_and(now, inside(zz)))
                    def _():
                        logits_unit(q, zz)

                    return carry

                lax.fori_loop(0, 2 * line, unit, 0)

                @pl.when(w == unit_slot(q, line - 1))
                def _():
                    send_stats(q)

            @pl.when(w == slopes_slot(q))
            def _():
                make_slopes(q)

                @pl.when(q == chunks - 1)
                def _():
                    lossall[0] = num[...]
                    for far in range(1, ways):
                        loss_copy(far).start()

            @pl.when(w == slopes_slot(q) + OWN)
            def _():
                add_gradient(first(q, 0), s_own.at[q], q == 0, False)

            @pl.when(w == got_slot(q))
            def _():
                for far in range(1, ways):
                    i = second(q, far)
                    slope_copy(q, ways - far).wait_recv()

                    def arrived(j, carry, i=i):
                        beside(i, 2 * j + sibling).wait_recv()
                        return carry

                    lax.fori_loop(0, 2 * line, arrived, 0)
                    add_gradient(i, s_got.at[far - 1, q], False, jnp.logical_and(q == final, far == ways - 1))

            return carry

        lax.fori_loop(0, chunks, chunk, 0)
        return carry

    lax.fori_loop(0, slots, slot, 0)

    out_copy(blocks - 1).start()
    for far in range(1, ways):
        loss_copy(far).wait_recv()
    result = jnp.zeros((8, LANES), f32)
    for s in range(steps):
        numerator = jnp.zeros((8, LANES), f32)
        for p in range(ways):
            for sub in range(split):
                numerator = numerator + lossall[p, s * split + sub]
        counted = jnp.sum(
            jnp.sum(count[s], axis=0, keepdims=True), axis=1, keepdims=True
        )
        result = result + step_decay**s * numerator / jnp.broadcast_to(counted, (8, LANES))
    loss[...] = result[0:1, 0:1]

    lax.fori_loop(drained, pieces, drain, 0)
    for j in range(blocks):
        out_copy(j).wait()
    for j in range(1, n):
        token_copy(j).wait_send()
    for far in range(1, ways):
        square_copy(far).wait_send()
        w_copy(far).wait_send()
        loss_copy(far).wait_send()
    for q in range(chunks):
        for j in range(1, n):
            stat_copy(q, j).wait_send()
        for far in range(1, ways):
            x_copy(q, far).wait_send()
            slope_copy(q, far).wait_send()


def head_step(hidden, gain, weight, labels, mask, offsets):
    steps, rows, width = hidden.shape
    vocab = weight.shape[1]
    n, ways = lax.axis_size("dp"), lax.axis_size("tensor")
    each = rows // ways
    split = SPLIT if each % (16 * SPLIT) == 0 else 1
    few = each // split
    chunks = steps * split
    pieces = chunks * (2 * ways - 1)
    vmem = pl.BlockSpec(memory_space=pltpu.VMEM)
    smem = pl.BlockSpec(memory_space=pltpu.SMEM)
    hbm = pl.BlockSpec(memory_space=pl.ANY)
    dma = pltpu.SemaphoreType.DMA
    f32, bf16 = jnp.float32, jnp.bfloat16
    return pl.pallas_call(
        functools.partial(head_kernel, n, ways),
        out_shape=[
            jax.ShapeDtypeStruct((width, vocab), f32),
            jax.ShapeDtypeStruct((1, 1), f32),
        ],
        in_specs=[hbm, vmem, hbm, vmem, vmem, smem],
        out_specs=[hbm, vmem],
        scratch_shapes=[
            pltpu.VMEM((width, vocab), f32),
            pltpu.VMEM((steps, rows, width), bf16),
            pltpu.VMEM((pieces, n, few, width), bf16),
            pltpu.VMEM((ways, width, vocab), bf16),
            pltpu.VMEM((chunks, n, few, vocab), f32),
            pltpu.VMEM((chunks, n, few, vocab), bf16),
            pltpu.VMEM((ways - 1, chunks, n, few, vocab), bf16),
            pltpu.VMEM((steps, n * rows, LANES), f32),
            pltpu.VMEM((steps, n * rows, LANES), f32),
            pltpu.VMEM((chunks, n * few, LANES), f32),
            pltpu.VMEM((n, 8, rows), jnp.int32),
            pltpu.VMEM((chunks, n, 2, 8, LANES), f32),
            pltpu.VMEM((chunks, 8, LANES), f32),
            pltpu.VMEM((chunks, 8, LANES), f32),
            pltpu.VMEM((chunks, 8, LANES), f32),
            pltpu.VMEM((steps, 8, rows), f32),
            pltpu.VMEM((ways, steps, 8, rows), f32),
            pltpu.VMEM((steps, rows, LANES), f32),
            pltpu.VMEM((ways, chunks, 8, LANES), f32),
            dma((4, pieces, n // 2)),
            dma((pieces, n)),
            dma((chunks, ways - 1)),
            dma((ways - 1,)),
            dma((ways - 1,)),
            dma((ways - 1,)),
            dma((ways - 1,)),
            dma((chunks, n)),
            dma((chunks, n)),
            dma((n,)),
            dma((n,)),
            dma((ways - 1, chunks)),
            dma((ways - 1, chunks)),
            dma((ways - 1,)),
            dma((ways - 1,)),
            dma((2,)),
            dma((width // LANES,)),
        ],
        compiler_params=pltpu.CompilerParams(
            collective_id=7, has_side_effects=True, vmem_limit_bytes=60 * 1024 * 1024
        ),
        name="head_step",
    )(hidden, gain, weight, labels, mask, offsets)


def local(drafter_hidden, norm_gain, head_weight, labels, loss_mask, offsets):
    gradient, loss = head_step(
        drafter_hidden, norm_gain, head_weight, labels[None], loss_mask[None], offsets
    )
    return (loss[0, 0], gradient)


def solution(mesh):
    return jax.shard_map(
        local,
        mesh=mesh,
        in_specs=(P(None, "dp", "tensor"), P("tensor"), P("tensor", "dp"), P("dp"), P("dp"), P()),
        out_specs=(P(), P("tensor", "dp")),
        check_vma=False,
    )
```

```python
import functools

import jax
import jax.numpy as jnp
from jax import lax
from jax.experimental import pallas as pl
from jax.experimental.pallas import tpu as pltpu
from jax.sharding import PartitionSpec as P

WINDOW = 512
MAXOFF = 4
LANES = 128

epsilon = 1e-05
step_decay = 0.8
MESH = pl.DeviceIdType.MESH

SPLIT = 2
GAP = 3
SPACE = 3
UNIT = 1
LAG = 3
OWN = 6
EARLY = 1
HOLD = 18


def rows_to_columns(row):
    return jnp.transpose(jnp.broadcast_to(row, (LANES, row.shape[1])))


def head_kernel(
    n, ways, x_in, gain, w_in, labels, mask, offsets, grad_out, loss,
    grad, xv, held, wall, logits, s_own, s_got, labcol, wcol, lcol, tok, statall, lserow, labpart, num,
    count, sqall, invcol, lossall,
    send, recv, xsend, wsend, wrecv, sqsend, sqrecv, ssend, srecv, tsend, trecv, gsend, grecv,
    lsend, lrecv, local_sem, out_sem,
):
    steps, rows, width = xv.shape
    vocab = w_in.shape[1]
    pieces, few = held.shape[0], held.shape[2]
    each = rows // ways
    split = each // few
    chunks = steps * split
    line = n // 4
    chunk_rows = n * few
    groups = chunk_rows // LANES
    main = chunks * ways
    me, rank = lax.axis_index("dp"), lax.axis_index("tensor")
    c, x, z = lax.rem(me, 2), lax.rem(me // 2, 2), me // 4
    sibling, other = 1 - c, 1 - x
    f32 = jnp.float32

    def at(z_, x_, c_):
        return (z_ * 2 + x_) * 2 + c_

    def first(q, p):
        return q * ways + p

    def second(q, far):
        return main + q * (ways - 1) + far - 1

    x_load = pltpu.make_async_copy(x_in, xv, local_sem.at[0])
    x_load.start()
    w_load = pltpu.make_async_copy(w_in, wall.at[0], local_sem.at[1])
    w_load.start()

    barrier = pltpu.get_barrier_semaphore()
    for j in range(1, n):
        pl.semaphore_signal(
            barrier, inc=1, device_id={"dp": lax.rem(me + j, n)}, device_id_type=MESH
        )
    for j in range(1, ways):
        pl.semaphore_signal(
            barrier, inc=1, device_id={"tensor": lax.rem(rank + j, ways)}, device_id_type=MESH
        )

    def to_tensor(src, dst, send_sem, recv_sem, far):
        return pltpu.make_async_remote_copy(
            src_ref=src,
            dst_ref=dst,
            send_sem=send_sem,
            recv_sem=recv_sem,
            device_id={"tensor": lax.rem(rank + far, ways)},
            device_id_type=MESH,
        )

    def to_dp(src, dst, send_sem, recv_sem, target):
        return pltpu.make_async_remote_copy(
            src_ref=src,
            dst_ref=dst,
            send_sem=send_sem,
            recv_sem=recv_sem,
            device_id={"dp": target},
            device_id_type=MESH,
        )

    def square_copy(far):
        return to_tensor(
            sqall.at[0], sqall.at[ways - far], sqsend.at[far - 1], sqrecv.at[ways - far - 1], far
        )

    def w_copy(far):
        return to_tensor(
            w_in, wall.at[ways - far], wsend.at[far - 1], wrecv.at[ways - far - 1], far
        )

    def x_copy(q, far):
        target = first(q, ways - far)
        return to_tensor(
            held.at[second(q, far), me],
            held.at[target, me],
            xsend.at[q, far - 1],
            recv.at[target, me],
            far,
        )

    def slope_copy(q, far):
        return to_tensor(
            s_own.at[q],
            s_got.at[ways - far - 1, q],
            gsend.at[far - 1, q],
            grecv.at[ways - far - 1, q],
            far,
        )

    def loss_copy(far):
        return to_tensor(
            lossall.at[0], lossall.at[ways - far], lsend.at[far - 1], lrecv.at[ways - far - 1], far
        )

    def token_copy(j):
        target = lax.rem(me + j, n)
        return to_dp(tok.at[me], tok.at[me], tsend.at[j], trecv.at[me], target)

    def token_wait(j):
        source = lax.rem(me + j, n)
        return to_dp(tok.at[source], tok.at[source], tsend.at[j], trecv.at[source], source)

    def stat_copy(q, j):
        target = lax.rem(me + j, n)
        return to_dp(
            statall.at[q, me], statall.at[q, me], ssend.at[q, j], srecv.at[q, me], target
        )

    def stat_wait(q, j):
        source = lax.rem(me + j, n)
        return to_dp(
            statall.at[q, source], statall.at[q, source], ssend.at[q, j], srecv.at[q, source], source
        )

    def block_copy(kind, i, b, target):
        return to_dp(held.at[i, b], held.at[i, b], send.at[kind, i, b // 2], recv.at[i, b], target)

    def ups(i, b):
        return block_copy(0, i, b, at(z + 1, x, c))

    def downs(i, b):
        return block_copy(1, i, b, at(z - 1, x, c))

    def across(i, b):
        return block_copy(2, i, b, at(z, other, c))

    def beside(i, b):
        return block_copy(3, i, b, at(z, x, sibling))

    def inside(zz):
        return jnp.logical_and(zz >= 0, zz < line)

    top_half = lax.broadcasted_iota(jnp.int32, (8, rows), 0) < 4
    tok[me] = jnp.where(
        top_half,
        jnp.broadcast_to(labels[...], (8, rows)),
        jnp.broadcast_to(mask[...], (8, rows)),
    )
    x_load.wait()
    for s in range(steps):

        def square(j, acc):
            part = xv[s, :, pl.ds(pl.multiple_of(j * LANES, LANES), LANES)].astype(f32)
            return acc + part * part

        acc = lax.fori_loop(0, width // LANES, square, jnp.zeros((rows, LANES), f32))
        column = jnp.sum(acc, axis=1, keepdims=True)
        flat = jnp.transpose(jnp.broadcast_to(column, (rows, LANES)))
        sqall[0, s] = flat[0:8]

    peers = n - 1 + ways - 1
    pl.semaphore_wait(barrier, peers)
    for far in range(1, ways):
        square_copy(far).start()
    for j in range(1, n):
        token_copy(j).start()
    labpart[...] = jnp.zeros_like(labpart)
    num[...] = jnp.zeros_like(num)
    count[...] = jnp.zeros_like(count)
    statall[:, me] = jnp.zeros((chunks, 2, 8, LANES), f32)
    for far in range(1, ways):
        square_copy(far).wait_recv()
    for s in range(steps):
        total = sqall[0, s]
        for p in range(1, ways):
            total = total + sqall[p, s]
        inverse = lax.rsqrt(total / (width * ways) + epsilon)
        invcol[s] = rows_to_columns(inverse[0:1])

    for s in range(steps):
        for far in range(ways):
            owner = lax.rem(rank + far, ways)
            offset = pl.multiple_of(owner * each, each)
            scale = jnp.concatenate([invcol[s, pl.ds(offset, each)]] * 2, axis=1)

            def normalise(j, carry, s=s, far=far, offset=offset, scale=scale):
                at_lane = pl.ds(pl.multiple_of(j * 2 * LANES, 2 * LANES), 2 * LANES)
                wide = xv[s, pl.ds(offset, each), at_lane].astype(f32)
                value = (wide * scale * gain[at_lane].astype(f32)[None]).astype(jnp.bfloat16)
                for sub in range(split):
                    q = s * split + sub
                    i = second(q, far) if far else first(q, 0)
                    held[i, me, :, at_lane] = value[sub * few : (sub + 1) * few]
                return carry

            lax.fori_loop(0, width // (2 * LANES), normalise, 0)
    for q in range(chunks):
        for far in range(1, ways):
            x_copy(q, far).start()
    for far in range(1, ways):
        w_copy(far).start()

    def relay(k, t):
        j = lax.rem(t, GAP * ways)
        i = ways * (t // (GAP * ways)) + j
        valid = jnp.logical_and(jnp.logical_and(t >= 0, j < ways), i < pieces)
        early = lax.rem(i, 6) == EARLY
        foreign = jnp.logical_and(i < main, lax.rem(i, ways) > 0)

        def along(zz, b):
            @pl.when(jnp.logical_and(zz <= z, z < line - 1))
            def _():
                ups(i, b).start()

            @pl.when(jnp.logical_and(zz >= z, z > 0))
            def _():
                downs(i, b).start()

        for side in (0, 1):
            zz = z + k if side else z - k
            ok = jnp.logical_and(inside(zz), k >= side)

            @pl.when(jnp.logical_and(valid, ok))
            def _(zz=zz):
                b = at(zz, x, c)

                @pl.when(jnp.logical_or(k > 0, foreign))
                def _():
                    beside(i, b).wait_recv()

                along(zz, b)

                @pl.when(jnp.logical_or(k == 0, jnp.logical_not(early)))
                def _():
                    across(i, b).start()

                beside(i, b).start()

        for side in (0, 1):
            zz = z + (k - 1) if side else z - (k - 1)
            ok = jnp.logical_and(inside(zz), k > side)

            @pl.when(jnp.logical_and(valid, ok))
            def _(zz=zz):
                b = at(zz, other, c)
                beside(i, b).wait_recv()

                @pl.when(early)
                def _():
                    along(zz, b)

                beside(i, b).start()

    def drain(i, carry):
        early = lax.rem(i, 6) == EARLY

        def one(zz, carry):
            own, far_side = at(zz, x, c), at(zz, other, c)
            up = jnp.logical_and(zz <= z, z < line - 1)
            down = jnp.logical_and(zz >= z, z > 0)
            beside(i, own).wait_send()
            beside(i, far_side).wait_send()

            @pl.when(up)
            def _():
                ups(i, own).wait_send()

            @pl.when(down)
            def _():
                downs(i, own).wait_send()

            @pl.when(jnp.logical_or(zz == z, jnp.logical_not(early)))
            def _():
                across(i, own).wait_send()

            @pl.when(early)
            def _():
                @pl.when(up)
                def _():
                    ups(i, far_side).wait_send()

                @pl.when(down)
                def _():
                    downs(i, far_side).wait_send()

            return carry

        lax.fori_loop(0, line, one, 0)
        return carry

    def token_block(b):
        here = tok[b].astype(f32)
        following = tok[jnp.minimum(b + 1, n - 1)].astype(f32)
        last = jnp.broadcast_to(here[:, rows - 1 : rows], (8, rows))
        following = jnp.where(b == n - 1, last, following)
        lane = lax.broadcasted_iota(jnp.int32, (8, rows), 1)
        position = lax.rem(b * rows + lane, WINDOW)
        for s in range(steps):
            by = offsets[s]
            chosen = here
            for far in range(1, MAXOFF + 1):
                shifted = jnp.where(
                    lane < rows - far,
                    pltpu.roll(here, rows - far, 1),
                    pltpu.roll(following, rows - far, 1),
                )
                chosen = jnp.where(by == far, shifted, chosen)
            weight = jnp.where(position + by < WINDOW, chosen, 0.0)[4:5]
            count[s, 0:1] = count[s, 0:1] + weight
            span = pl.ds(pl.multiple_of(b * rows, rows), rows)
            labcol[s, span] = rows_to_columns(chosen[0:1])
            wcol[s, span] = rows_to_columns(weight)

    def tokens(q, b):
        start = b * rows + rank * each + lax.rem(q, split) * few
        return q // split, pl.ds(pl.multiple_of(start, few), few)

    def hits(q, b, chunk):
        columns = (
            me * vocab + chunk * LANES + lax.broadcasted_iota(jnp.int32, (few, LANES), 1)
        ).astype(f32)
        return labcol[tokens(q, b)] == columns

    def folded(values):
        return jnp.sum(values.reshape(few // 8, 8, LANES), axis=0)

    def logits_unit(q, zz):
        acc = None
        for p in range(ways):
            for core_x in range(2):
                beside(first(q, p), at(zz, core_x, sibling)).wait_recv()
        for p in range(ways):
            lhs = held[first(q, p), pl.ds(4 * zz, 4)].reshape(4 * few, width)
            part = jnp.dot(lhs, wall[p], preferred_element_type=f32)
            acc = part if acc is None else acc + part
        logits[q, pl.ds(4 * zz, 4)] = acc.reshape(4, few, vocab)

        def block_stats(j, carry):
            b = 4 * zz + j
            span = pl.ds(pl.multiple_of(b * few, few), few)
            tile = logits[q, b]
            top = jnp.max(tile, axis=1, keepdims=True)
            lse = top + jnp.log(jnp.sum(jnp.exp(tile - top), axis=1, keepdims=True))
            lcol[q, span] = jnp.broadcast_to(lse, (few, LANES))
            found = jnp.zeros((few, LANES), f32)
            for chunk in range(vocab // LANES):
                part = tile[:, chunk * LANES : (chunk + 1) * LANES]
                found = found + jnp.where(hits(q, b, chunk), part, 0.0)
            labpart[q] = labpart[q] + folded(wcol[tokens(q, b)] * found)
            return carry

        lax.fori_loop(0, 4, block_stats, 0)

    def send_stats(q):
        def group(g, carry):
            tile = lcol[q, pl.ds(pl.multiple_of(g * LANES, LANES), LANES)]
            statall[q, me, 0, pl.ds(g, 1)] = jnp.transpose(tile)[0:1]
            return carry

        lax.fori_loop(0, groups, group, 0)
        statall[q, me, 1] = labpart[q]
        for j in range(1, n):
            stat_copy(q, j).start()

    def make_slopes(q):
        for j in range(1, n):
            stat_wait(q, j).wait_recv()

        def highest(j, top):
            return jnp.maximum(top, statall[q, j, 0])

        top = lax.fori_loop(1, n, highest, statall[q, 0, 0])

        def sums(j, carry):
            total, found = carry
            return total + jnp.exp(statall[q, j, 0] - top), found + statall[q, j, 1]

        zero = jnp.zeros((8, LANES), f32)
        total, found = lax.fori_loop(0, n, sums, (zero, zero))
        lserow[q] = top + jnp.log(total)

        def group(g, carry):
            span = pl.ds(pl.multiple_of(g * LANES, LANES), LANES)
            lcol[q, span] = rows_to_columns(lserow[q, pl.ds(g, 1)])
            return carry

        lax.fori_loop(0, groups, group, 0)
        factor = jnp.float32(1.0)
        for s in range(1, steps):
            factor = jnp.where(q // split == s, jnp.float32(step_decay**s), factor)

        def block(b, carry):
            span = pl.ds(pl.multiple_of(b * few, few), few)
            lse = lcol[q, span]
            weight = wcol[tokens(q, b)]
            scale = factor * weight
            for chunk in range(vocab // LANES):
                lanes = pl.ds(chunk * LANES, LANES)
                softmax = jnp.exp(logits[q, b, :, lanes] - lse)
                hit = jnp.where(hits(q, b, chunk), 1.0, 0.0)
                s_own[q, b, :, lanes] = (scale * (softmax - hit)).astype(jnp.bfloat16)
            return carry + folded(weight * lse)

        weighted = lax.fori_loop(0, n, block, zero)
        for far in range(1, ways):
            slope_copy(q, far).start()
        numerator = jnp.sum(weighted, axis=0, keepdims=True) - jnp.sum(
            jnp.sum(found, axis=0, keepdims=True), axis=1, keepdims=True
        )
        num[q] = jnp.broadcast_to(numerator, (8, LANES))

    block = 512 if width % 512 == 0 else LANES
    blocks = width // block

    def out_copy(j):
        lanes = pl.ds(pl.multiple_of(j * block, block), block)
        return pltpu.make_async_copy(grad.at[lanes], grad_out.at[lanes], out_sem.at[j])

    def add_gradient(i, slopes, first_time, last_time):

        def part(j, carry):
            lanes = pl.ds(pl.multiple_of(j * block, block), block)
            lhs = held[i, :, :, lanes].reshape(chunk_rows, block)
            rhs = slopes[...].reshape(chunk_rows, vocab)
            value = lax.dot_general(
                lhs, rhs, (((0,), (0,)), ((), ())), preferred_element_type=f32
            )

            @pl.when(first_time)
            def _():
                grad[lanes, :] = value

            @pl.when(jnp.logical_not(first_time))
            def _():
                grad[lanes, :] = grad[lanes, :] + value

            @pl.when(jnp.logical_and(last_time, j > 0))
            def _():
                out_copy(j - 1).start()

            return carry

        lax.fori_loop(0, blocks, part, 0)

    def larger(a, b):
        both = isinstance(a, int) and isinstance(b, int)
        return max(a, b) if both else jnp.maximum(a, b)

    def ready(i, k):
        return GAP * ways * (i // ways) + i % ways + SPACE * k

    def unit_slot(q, u):
        held_back = HOLD + q * line + u - 1000 * (q // split)
        return larger(ready(q * ways + ways - 1, u + 1) + UNIT, larger(held_back, HOLD))

    def slopes_slot(q):
        return unit_slot(q, line - 1) + LAG

    def got_slot(q):
        return larger(ready(second(q, ways - 1), line), slopes_slot(q)) + 1

    final = chunks - 1
    slots = 1 + max(ready(pieces - 1, line), slopes_slot(final) + OWN, got_slot(final))
    assert slopes_slot(0) + OWN < got_slot(0) and slopes_slot(final) + OWN < got_slot(final)
    assert all(unit_slot(q, 0) >= unit_slot(0, 0) for q in range(chunks))
    drained = sum(ready(i, line + 2) < slots for i in range(pieces))

    def slot(w, carry):
        for k in range(line, -1, -1):
            relay(k, w - SPACE * k)
        t = w - SPACE * (line + 2)
        i = ways * (t // (GAP * ways)) + lax.rem(t, GAP * ways)

        @pl.when(jnp.logical_and(t >= 0, jnp.logical_and(lax.rem(t, GAP * ways) < ways, i < drained)))
        def _():
            drain(i, 0)

        @pl.when(jnp.logical_and(w >= 1, w <= n))
        def _():
            @pl.when(w == 1)
            def _():
                for j in range(1, n):
                    token_wait(j).wait_recv()

            token_block(w - 1)

        @pl.when(w == unit_slot(0, 0))
        def _():
            w_load.wait()
            for far in range(1, ways):
                w_copy(far).wait_recv()

        def chunk(q, carry):
            @pl.when(jnp.logical_and(w >= unit_slot(q, 0), w <= unit_slot(q, line - 1)))
            def _():
                def unit(v, carry):
                    u, side = v // 2, lax.rem(v, 2)
                    zz = z + u * (2 * side - 1)
                    now = jnp.logical_and(w == unit_slot(q, u), u >= side)

                    @pl.when(jnp.logical_and(now, inside(zz)))
                    def _():
                        logits_unit(q, zz)

                    return carry

                lax.fori_loop(0, 2 * line, unit, 0)

                @pl.when(w == unit_slot(q, line - 1))
                def _():
                    send_stats(q)

            @pl.when(w == slopes_slot(q))
            def _():
                make_slopes(q)

                @pl.when(q == chunks - 1)
                def _():
                    lossall[0] = num[...]
                    for far in range(1, ways):
                        loss_copy(far).start()

            @pl.when(w == slopes_slot(q) + OWN)
            def _():
                add_gradient(first(q, 0), s_own.at[q], q == 0, False)

            @pl.when(w == got_slot(q))
            def _():
                for far in range(1, ways):
                    i = second(q, far)
                    slope_copy(q, ways - far).wait_recv()

                    def arrived(j, carry, i=i):
                        beside(i, 2 * j + sibling).wait_recv()
                        return carry

                    lax.fori_loop(0, 2 * line, arrived, 0)
                    add_gradient(i, s_got.at[far - 1, q], False, jnp.logical_and(q == final, far == ways - 1))

            return carry

        lax.fori_loop(0, chunks, chunk, 0)
        return carry

    lax.fori_loop(0, slots, slot, 0)

    out_copy(blocks - 1).start()
    for far in range(1, ways):
        loss_copy(far).wait_recv()
    result = jnp.zeros((8, LANES), f32)
    for s in range(steps):
        numerator = jnp.zeros((8, LANES), f32)
        for p in range(ways):
            for sub in range(split):
                numerator = numerator + lossall[p, s * split + sub]
        counted = jnp.sum(
            jnp.sum(count[s], axis=0, keepdims=True), axis=1, keepdims=True
        )
        result = result + step_decay**s * numerator / jnp.broadcast_to(counted, (8, LANES))
    loss[...] = result[0:1, 0:1]

    lax.fori_loop(drained, pieces, drain, 0)
    for j in range(blocks):
        out_copy(j).wait()
    for j in range(1, n):
        token_copy(j).wait_send()
    for far in range(1, ways):
        square_copy(far).wait_send()
        w_copy(far).wait_send()
        loss_copy(far).wait_send()
    for q in range(chunks):
        for j in range(1, n):
            stat_copy(q, j).wait_send()
        for far in range(1, ways):
            x_copy(q, far).wait_send()
            slope_copy(q, far).wait_send()


def head_step(hidden, gain, weight, labels, mask, offsets):
    steps, rows, width = hidden.shape
    vocab = weight.shape[1]
    n, ways = lax.axis_size("dp"), lax.axis_size("tensor")
    each = rows // ways
    split = SPLIT if each % (16 * SPLIT) == 0 else 1
    few = each // split
    chunks = steps * split
    pieces = chunks * (2 * ways - 1)
    vmem = pl.BlockSpec(memory_space=pltpu.VMEM)
    smem = pl.BlockSpec(memory_space=pltpu.SMEM)
    hbm = pl.BlockSpec(memory_space=pl.ANY)
    dma = pltpu.SemaphoreType.DMA
    f32, bf16 = jnp.float32, jnp.bfloat16
    return pl.pallas_call(
        functools.partial(head_kernel, n, ways),
        out_shape=[
            jax.ShapeDtypeStruct((width, vocab), f32),
            jax.ShapeDtypeStruct((1, 1), f32),
        ],
        in_specs=[hbm, vmem, hbm, vmem, vmem, smem],
        out_specs=[hbm, vmem],
        scratch_shapes=[
            pltpu.VMEM((width, vocab), f32),
            pltpu.VMEM((steps, rows, width), bf16),
            pltpu.VMEM((pieces, n, few, width), bf16),
            pltpu.VMEM((ways, width, vocab), bf16),
            pltpu.VMEM((chunks, n, few, vocab), f32),
            pltpu.VMEM((chunks, n, few, vocab), bf16),
            pltpu.VMEM((ways - 1, chunks, n, few, vocab), bf16),
            pltpu.VMEM((steps, n * rows, LANES), f32),
            pltpu.VMEM((steps, n * rows, LANES), f32),
            pltpu.VMEM((chunks, n * few, LANES), f32),
            pltpu.VMEM((n, 8, rows), jnp.int32),
            pltpu.VMEM((chunks, n, 2, 8, LANES), f32),
            pltpu.VMEM((chunks, 8, LANES), f32),
            pltpu.VMEM((chunks, 8, LANES), f32),
            pltpu.VMEM((chunks, 8, LANES), f32),
            pltpu.VMEM((steps, 8, rows), f32),
            pltpu.VMEM((ways, steps, 8, rows), f32),
            pltpu.VMEM((steps, rows, LANES), f32),
            pltpu.VMEM((ways, chunks, 8, LANES), f32),
            dma((4, pieces, n // 2)),
            dma((pieces, n)),
            dma((chunks, ways - 1)),
            dma((ways - 1,)),
            dma((ways - 1,)),
            dma((ways - 1,)),
            dma((ways - 1,)),
            dma((chunks, n)),
            dma((chunks, n)),
            dma((n,)),
            dma((n,)),
            dma((ways - 1, chunks)),
            dma((ways - 1, chunks)),
            dma((ways - 1,)),
            dma((ways - 1,)),
            dma((2,)),
            dma((width // LANES,)),
        ],
        compiler_params=pltpu.CompilerParams(
            collective_id=7, has_side_effects=True, vmem_limit_bytes=60 * 1024 * 1024
        ),
        name="head_step",
    )(hidden, gain, weight, labels, mask, offsets)


def local(drafter_hidden, norm_gain, head_weight, labels, loss_mask, offsets):
    gradient, loss = head_step(
        drafter_hidden, norm_gain, head_weight, labels[None], loss_mask[None], offsets
    )
    return (loss[0, 0], gradient)


def solution(mesh):
    return jax.shard_map(
        local,
        mesh=mesh,
        in_specs=(P(None, "dp", "tensor"), P("tensor"), P("tensor", "dp"), P("dp"), P("dp"), P()),
        out_specs=(P(), P("tensor", "dp")),
        check_vma=False,
    )
```

```python
import functools

import jax
import jax.numpy as jnp
from jax import lax
from jax.experimental import pallas as pl
from jax.experimental.pallas import tpu as pltpu
from jax.sharding import PartitionSpec as P

WINDOW = 512
MAXOFF = 4
LANES = 128

epsilon = 1e-05
step_decay = 0.8
MESH = pl.DeviceIdType.MESH

SPLIT = 2
GAP = 3
SPACE = 3
UNIT = 1
LAG = 4
OWN = 5
EARLY = 1
HOLD = 18


def rows_to_columns(row):
    return jnp.transpose(jnp.broadcast_to(row, (LANES, row.shape[1])))


def head_kernel(
    n, ways, x_in, gain, w_in, labels, mask, offsets, grad_out, loss,
    grad, xv, held, wall, logits, s_own, s_got, labcol, wcol, lcol, tok, statall, lserow, labpart, num,
    count, sqall, invcol, lossall,
    send, recv, xsend, wsend, wrecv, sqsend, sqrecv, ssend, srecv, tsend, trecv, gsend, grecv,
    lsend, lrecv, local_sem, out_sem,
):
    steps, rows, width = xv.shape
    vocab = w_in.shape[1]
    pieces, few = held.shape[0], held.shape[2]
    each = rows // ways
    split = each // few
    chunks = steps * split
    line = n // 4
    chunk_rows = n * few
    groups = chunk_rows // LANES
    main = chunks * ways
    me, rank = lax.axis_index("dp"), lax.axis_index("tensor")
    c, x, z = lax.rem(me, 2), lax.rem(me // 2, 2), me // 4
    sibling, other = 1 - c, 1 - x
    f32 = jnp.float32

    def at(z_, x_, c_):
        return (z_ * 2 + x_) * 2 + c_

    def first(q, p):
        return q * ways + p

    def second(q, far):
        return main + q * (ways - 1) + far - 1

    x_load = pltpu.make_async_copy(x_in, xv, local_sem.at[0])
    x_load.start()
    w_load = pltpu.make_async_copy(w_in, wall.at[0], local_sem.at[1])
    w_load.start()

    barrier = pltpu.get_barrier_semaphore()
    for j in range(1, n):
        pl.semaphore_signal(
            barrier, inc=1, device_id={"dp": lax.rem(me + j, n)}, device_id_type=MESH
        )
    for j in range(1, ways):
        pl.semaphore_signal(
            barrier, inc=1, device_id={"tensor": lax.rem(rank + j, ways)}, device_id_type=MESH
        )

    def to_tensor(src, dst, send_sem, recv_sem, far):
        return pltpu.make_async_remote_copy(
            src_ref=src,
            dst_ref=dst,
            send_sem=send_sem,
            recv_sem=recv_sem,
            device_id={"tensor": lax.rem(rank + far, ways)},
            device_id_type=MESH,
        )

    def to_dp(src, dst, send_sem, recv_sem, target):
        return pltpu.make_async_remote_copy(
            src_ref=src,
            dst_ref=dst,
            send_sem=send_sem,
            recv_sem=recv_sem,
            device_id={"dp": target},
            device_id_type=MESH,
        )

    def square_copy(far):
        return to_tensor(
            sqall.at[0], sqall.at[ways - far], sqsend.at[far - 1], sqrecv.at[ways - far - 1], far
        )

    def w_copy(far):
        return to_tensor(
            w_in, wall.at[ways - far], wsend.at[far - 1], wrecv.at[ways - far - 1], far
        )

    def x_copy(q, far):
        target = first(q, ways - far)
        return to_tensor(
            held.at[second(q, far), me],
            held.at[target, me],
            xsend.at[q, far - 1],
            recv.at[target, me],
            far,
        )

    def slope_copy(q, far):
        return to_tensor(
            s_own.at[q],
            s_got.at[ways - far - 1, q],
            gsend.at[far - 1, q],
            grecv.at[ways - far - 1, q],
            far,
        )

    def loss_copy(far):
        return to_tensor(
            lossall.at[0], lossall.at[ways - far], lsend.at[far - 1], lrecv.at[ways - far - 1], far
        )

    def token_copy(j):
        target = lax.rem(me + j, n)
        return to_dp(tok.at[me], tok.at[me], tsend.at[j], trecv.at[me], target)

    def token_wait(j):
        source = lax.rem(me + j, n)
        return to_dp(tok.at[source], tok.at[source], tsend.at[j], trecv.at[source], source)

    def stat_copy(q, j):
        target = lax.rem(me + j, n)
        return to_dp(
            statall.at[q, me], statall.at[q, me], ssend.at[q, j], srecv.at[q, me], target
        )

    def stat_wait(q, j):
        source = lax.rem(me + j, n)
        return to_dp(
            statall.at[q, source], statall.at[q, source], ssend.at[q, j], srecv.at[q, source], source
        )

    def block_copy(kind, i, b, target):
        return to_dp(held.at[i, b], held.at[i, b], send.at[kind, i, b // 2], recv.at[i, b], target)

    def ups(i, b):
        return block_copy(0, i, b, at(z + 1, x, c))

    def downs(i, b):
        return block_copy(1, i, b, at(z - 1, x, c))

    def across(i, b):
        return block_copy(2, i, b, at(z, other, c))

    def beside(i, b):
        return block_copy(3, i, b, at(z, x, sibling))

    def inside(zz):
        return jnp.logical_and(zz >= 0, zz < line)

    top_half = lax.broadcasted_iota(jnp.int32, (8, rows), 0) < 4
    tok[me] = jnp.where(
        top_half,
        jnp.broadcast_to(labels[...], (8, rows)),
        jnp.broadcast_to(mask[...], (8, rows)),
    )
    x_load.wait()
    for s in range(steps):

        def square(j, acc):
            part = xv[s, :, pl.ds(pl.multiple_of(j * LANES, LANES), LANES)].astype(f32)
            return acc + part * part

        acc = lax.fori_loop(0, width // LANES, square, jnp.zeros((rows, LANES), f32))
        column = jnp.sum(acc, axis=1, keepdims=True)
        flat = jnp.transpose(jnp.broadcast_to(column, (rows, LANES)))
        sqall[0, s] = flat[0:8]

    peers = n - 1 + ways - 1
    pl.semaphore_wait(barrier, peers)
    for far in range(1, ways):
        square_copy(far).start()
    for j in range(1, n):
        token_copy(j).start()
    labpart[...] = jnp.zeros_like(labpart)
    num[...] = jnp.zeros_like(num)
    count[...] = jnp.zeros_like(count)
    statall[:, me] = jnp.zeros((chunks, 2, 8, LANES), f32)
    for far in range(1, ways):
        square_copy(far).wait_recv()
    for s in range(steps):
        total = sqall[0, s]
        for p in range(1, ways):
            total = total + sqall[p, s]
        inverse = lax.rsqrt(total / (width * ways) + epsilon)
        invcol[s] = rows_to_columns(inverse[0:1])

    for s in range(steps):
        for far in range(ways):
            owner = lax.rem(rank + far, ways)
            offset = pl.multiple_of(owner * each, each)
            scale = jnp.concatenate([invcol[s, pl.ds(offset, each)]] * 2, axis=1)

            def normalise(j, carry, s=s, far=far, offset=offset, scale=scale):
                at_lane = pl.ds(pl.multiple_of(j * 2 * LANES, 2 * LANES), 2 * LANES)
                wide = xv[s, pl.ds(offset, each), at_lane].astype(f32)
                value = (wide * scale * gain[at_lane].astype(f32)[None]).astype(jnp.bfloat16)
                for sub in range(split):
                    q = s * split + sub
                    i = second(q, far) if far else first(q, 0)
                    held[i, me, :, at_lane] = value[sub * few : (sub + 1) * few]
                return carry

            lax.fori_loop(0, width // (2 * LANES), normalise, 0)
    for q in range(chunks):
        for far in range(1, ways):
            x_copy(q, far).start()
    for far in range(1, ways):
        w_copy(far).start()

    def relay(k, t):
        j = lax.rem(t, GAP * ways)
        i = ways * (t // (GAP * ways)) + j
        valid = jnp.logical_and(jnp.logical_and(t >= 0, j < ways), i < pieces)
        early = lax.rem(i, 6) == EARLY
        foreign = jnp.logical_and(i < main, lax.rem(i, ways) > 0)

        def along(zz, b):
            @pl.when(jnp.logical_and(zz <= z, z < line - 1))
            def _():
                ups(i, b).start()

            @pl.when(jnp.logical_and(zz >= z, z > 0))
            def _():
                downs(i, b).start()

        for side in (0, 1):
            zz = z + k if side else z - k
            ok = jnp.logical_and(inside(zz), k >= side)

            @pl.when(jnp.logical_and(valid, ok))
            def _(zz=zz):
                b = at(zz, x, c)

                @pl.when(jnp.logical_or(k > 0, foreign))
                def _():
                    beside(i, b).wait_recv()

                along(zz, b)

                @pl.when(jnp.logical_or(k == 0, jnp.logical_not(early)))
                def _():
                    across(i, b).start()

                beside(i, b).start()

        for side in (0, 1):
            zz = z + (k - 1) if side else z - (k - 1)
            ok = jnp.logical_and(inside(zz), k > side)

            @pl.when(jnp.logical_and(valid, ok))
            def _(zz=zz):
                b = at(zz, other, c)
                beside(i, b).wait_recv()

                @pl.when(early)
                def _():
                    along(zz, b)

                beside(i, b).start()

    def drain(i, carry):
        early = lax.rem(i, 6) == EARLY

        def one(zz, carry):
            own, far_side = at(zz, x, c), at(zz, other, c)
            up = jnp.logical_and(zz <= z, z < line - 1)
            down = jnp.logical_and(zz >= z, z > 0)
            beside(i, own).wait_send()
            beside(i, far_side).wait_send()

            @pl.when(up)
            def _():
                ups(i, own).wait_send()

            @pl.when(down)
            def _():
                downs(i, own).wait_send()

            @pl.when(jnp.logical_or(zz == z, jnp.logical_not(early)))
            def _():
                across(i, own).wait_send()

            @pl.when(early)
            def _():
                @pl.when(up)
                def _():
                    ups(i, far_side).wait_send()

                @pl.when(down)
                def _():
                    downs(i, far_side).wait_send()

            return carry

        lax.fori_loop(0, line, one, 0)
        return carry

    def token_block(b):
        here = tok[b].astype(f32)
        following = tok[jnp.minimum(b + 1, n - 1)].astype(f32)
        last = jnp.broadcast_to(here[:, rows - 1 : rows], (8, rows))
        following = jnp.where(b == n - 1, last, following)
        lane = lax.broadcasted_iota(jnp.int32, (8, rows), 1)
        position = lax.rem(b * rows + lane, WINDOW)
        for s in range(steps):
            by = offsets[s]
            chosen = here
            for far in range(1, MAXOFF + 1):
                shifted = jnp.where(
                    lane < rows - far,
                    pltpu.roll(here, rows - far, 1),
                    pltpu.roll(following, rows - far, 1),
                )
                chosen = jnp.where(by == far, shifted, chosen)
            weight = jnp.where(position + by < WINDOW, chosen, 0.0)[4:5]
            count[s, 0:1] = count[s, 0:1] + weight
            span = pl.ds(pl.multiple_of(b * rows, rows), rows)
            labcol[s, span] = rows_to_columns(chosen[0:1])
            wcol[s, span] = rows_to_columns(weight)

    def tokens(q, b):
        start = b * rows + rank * each + lax.rem(q, split) * few
        return q // split, pl.ds(pl.multiple_of(start, few), few)

    def hits(q, b, chunk):
        columns = (
            me * vocab + chunk * LANES + lax.broadcasted_iota(jnp.int32, (few, LANES), 1)
        ).astype(f32)
        return labcol[tokens(q, b)] == columns

    def folded(values):
        return jnp.sum(values.reshape(few // 8, 8, LANES), axis=0)

    def logits_unit(q, zz):
        acc = None
        for p in range(ways):
            for core_x in range(2):
                beside(first(q, p), at(zz, core_x, sibling)).wait_recv()
        for p in range(ways):
            lhs = held[first(q, p), pl.ds(4 * zz, 4)].reshape(4 * few, width)
            part = jnp.dot(lhs, wall[p], preferred_element_type=f32)
            acc = part if acc is None else acc + part
        logits[q, pl.ds(4 * zz, 4)] = acc.reshape(4, few, vocab)

        def block_stats(j, carry):
            b = 4 * zz + j
            span = pl.ds(pl.multiple_of(b * few, few), few)
            tile = logits[q, b]
            top = jnp.max(tile, axis=1, keepdims=True)
            lse = top + jnp.log(jnp.sum(jnp.exp(tile - top), axis=1, keepdims=True))
            lcol[q, span] = jnp.broadcast_to(lse, (few, LANES))
            found = jnp.zeros((few, LANES), f32)
            for chunk in range(vocab // LANES):
                part = tile[:, chunk * LANES : (chunk + 1) * LANES]
                found = found + jnp.where(hits(q, b, chunk), part, 0.0)
            labpart[q] = labpart[q] + folded(wcol[tokens(q, b)] * found)
            return carry

        lax.fori_loop(0, 4, block_stats, 0)

    def send_stats(q):
        def group(g, carry):
            tile = lcol[q, pl.ds(pl.multiple_of(g * LANES, LANES), LANES)]
            statall[q, me, 0, pl.ds(g, 1)] = jnp.transpose(tile)[0:1]
            return carry

        lax.fori_loop(0, groups, group, 0)
        statall[q, me, 1] = labpart[q]
        for j in range(1, n):
            stat_copy(q, j).start()

    def make_slopes(q):
        for j in range(1, n):
            stat_wait(q, j).wait_recv()

        def highest(j, top):
            return jnp.maximum(top, statall[q, j, 0])

        top = lax.fori_loop(1, n, highest, statall[q, 0, 0])

        def sums(j, carry):
            total, found = carry
            return total + jnp.exp(statall[q, j, 0] - top), found + statall[q, j, 1]

        zero = jnp.zeros((8, LANES), f32)
        total, found = lax.fori_loop(0, n, sums, (zero, zero))
        lserow[q] = top + jnp.log(total)

        def group(g, carry):
            span = pl.ds(pl.multiple_of(g * LANES, LANES), LANES)
            lcol[q, span] = rows_to_columns(lserow[q, pl.ds(g, 1)])
            return carry

        lax.fori_loop(0, groups, group, 0)
        factor = jnp.float32(1.0)
        for s in range(1, steps):
            factor = jnp.where(q // split == s, jnp.float32(step_decay**s), factor)

        def block(b, carry):
            span = pl.ds(pl.multiple_of(b * few, few), few)
            lse = lcol[q, span]
            weight = wcol[tokens(q, b)]
            scale = factor * weight
            for chunk in range(vocab // LANES):
                lanes = pl.ds(chunk * LANES, LANES)
                softmax = jnp.exp(logits[q, b, :, lanes] - lse)
                hit = jnp.where(hits(q, b, chunk), 1.0, 0.0)
                s_own[q, b, :, lanes] = (scale * (softmax - hit)).astype(jnp.bfloat16)
            return carry + folded(weight * lse)

        weighted = lax.fori_loop(0, n, block, zero)
        for far in range(1, ways):
            slope_copy(q, far).start()
        numerator = jnp.sum(weighted, axis=0, keepdims=True) - jnp.sum(
            jnp.sum(found, axis=0, keepdims=True), axis=1, keepdims=True
        )
        num[q] = jnp.broadcast_to(numerator, (8, LANES))

    block = 512 if width % 512 == 0 else LANES
    blocks = width // block

    def out_copy(j):
        lanes = pl.ds(pl.multiple_of(j * block, block), block)
        return pltpu.make_async_copy(grad.at[lanes], grad_out.at[lanes], out_sem.at[j])

    def add_gradient(i, slopes, first_time, last_time):

        def part(j, carry):
            lanes = pl.ds(pl.multiple_of(j * block, block), block)
            lhs = held[i, :, :, lanes].reshape(chunk_rows, block)
            rhs = slopes[...].reshape(chunk_rows, vocab)
            value = lax.dot_general(
                lhs, rhs, (((0,), (0,)), ((), ())), preferred_element_type=f32
            )

            @pl.when(first_time)
            def _():
                grad[lanes, :] = value

            @pl.when(jnp.logical_not(first_time))
            def _():
                grad[lanes, :] = grad[lanes, :] + value

            @pl.when(jnp.logical_and(last_time, j > 0))
            def _():
                out_copy(j - 1).start()

            return carry

        lax.fori_loop(0, blocks, part, 0)

    def larger(a, b):
        both = isinstance(a, int) and isinstance(b, int)
        return max(a, b) if both else jnp.maximum(a, b)

    def ready(i, k):
        return GAP * ways * (i // ways) + i % ways + SPACE * k

    def unit_slot(q, u):
        held_back = HOLD + q * line + u - 1000 * (q // split)
        return larger(ready(q * ways + ways - 1, u + 1) + UNIT, larger(held_back, HOLD))

    def slopes_slot(q):
        return unit_slot(q, line - 1) + LAG

    def got_slot(q):
        return larger(ready(second(q, ways - 1), line), slopes_slot(q)) + 1

    final = chunks - 1
    slots = 1 + max(ready(pieces - 1, line), slopes_slot(final) + OWN, got_slot(final))
    assert slopes_slot(0) + OWN < got_slot(0) and slopes_slot(final) + OWN < got_slot(final)
    assert all(unit_slot(q, 0) >= unit_slot(0, 0) for q in range(chunks))
    drained = sum(ready(i, line + 2) < slots for i in range(pieces))

    def slot(w, carry):
        for k in range(line, -1, -1):
            relay(k, w - SPACE * k)
        t = w - SPACE * (line + 2)
        i = ways * (t // (GAP * ways)) + lax.rem(t, GAP * ways)

        @pl.when(jnp.logical_and(t >= 0, jnp.logical_and(lax.rem(t, GAP * ways) < ways, i < drained)))
        def _():
            drain(i, 0)

        @pl.when(jnp.logical_and(w >= 1, w <= n))
        def _():
            @pl.when(w == 1)
            def _():
                for j in range(1, n):
                    token_wait(j).wait_recv()

            token_block(w - 1)

        @pl.when(w == unit_slot(0, 0))
        def _():
            w_load.wait()
            for far in range(1, ways):
                w_copy(far).wait_recv()

        def chunk(q, carry):
            @pl.when(jnp.logical_and(w >= unit_slot(q, 0), w <= unit_slot(q, line - 1)))
            def _():
                def unit(v, carry):
                    u, side = v // 2, lax.rem(v, 2)
                    zz = z + u * (2 * side - 1)
                    now = jnp.logical_and(w == unit_slot(q, u), u >= side)

                    @pl.when(jnp.logical_and(now, inside(zz)))
                    def _():
                        logits_unit(q, zz)

                    return carry

                lax.fori_loop(0, 2 * line, unit, 0)

                @pl.when(w == unit_slot(q, line - 1))
                def _():
                    send_stats(q)

            @pl.when(w == slopes_slot(q))
            def _():
                make_slopes(q)

                @pl.when(q == chunks - 1)
                def _():
                    lossall[0] = num[...]
                    for far in range(1, ways):
                        loss_copy(far).start()

            @pl.when(w == slopes_slot(q) + OWN)
            def _():
                add_gradient(first(q, 0), s_own.at[q], q == 0, False)

            @pl.when(w == got_slot(q))
            def _():
                for far in range(1, ways):
                    i = second(q, far)
                    slope_copy(q, ways - far).wait_recv()

                    def arrived(j, carry, i=i):
                        beside(i, 2 * j + sibling).wait_recv()
                        return carry

                    lax.fori_loop(0, 2 * line, arrived, 0)
                    add_gradient(i, s_got.at[far - 1, q], False, jnp.logical_and(q == final, far == ways - 1))

            return carry

        lax.fori_loop(0, chunks, chunk, 0)
        return carry

    lax.fori_loop(0, slots, slot, 0)

    out_copy(blocks - 1).start()
    for far in range(1, ways):
        loss_copy(far).wait_recv()
    result = jnp.zeros((8, LANES), f32)
    for s in range(steps):
        numerator = jnp.zeros((8, LANES), f32)
        for p in range(ways):
            for sub in range(split):
                numerator = numerator + lossall[p, s * split + sub]
        counted = jnp.sum(
            jnp.sum(count[s], axis=0, keepdims=True), axis=1, keepdims=True
        )
        result = result + step_decay**s * numerator / jnp.broadcast_to(counted, (8, LANES))
    loss[...] = result[0:1, 0:1]

    lax.fori_loop(drained, pieces, drain, 0)
    for j in range(blocks):
        out_copy(j).wait()
    for j in range(1, n):
        token_copy(j).wait_send()
    for far in range(1, ways):
        square_copy(far).wait_send()
        w_copy(far).wait_send()
        loss_copy(far).wait_send()
    for q in range(chunks):
        for j in range(1, n):
            stat_copy(q, j).wait_send()
        for far in range(1, ways):
            x_copy(q, far).wait_send()
            slope_copy(q, far).wait_send()


def head_step(hidden, gain, weight, labels, mask, offsets):
    steps, rows, width = hidden.shape
    vocab = weight.shape[1]
    n, ways = lax.axis_size("dp"), lax.axis_size("tensor")
    each = rows // ways
    split = SPLIT if each % (16 * SPLIT) == 0 else 1
    few = each // split
    chunks = steps * split
    pieces = chunks * (2 * ways - 1)
    vmem = pl.BlockSpec(memory_space=pltpu.VMEM)
    smem = pl.BlockSpec(memory_space=pltpu.SMEM)
    hbm = pl.BlockSpec(memory_space=pl.ANY)
    dma = pltpu.SemaphoreType.DMA
    f32, bf16 = jnp.float32, jnp.bfloat16
    return pl.pallas_call(
        functools.partial(head_kernel, n, ways),
        out_shape=[
            jax.ShapeDtypeStruct((width, vocab), f32),
            jax.ShapeDtypeStruct((1, 1), f32),
        ],
        in_specs=[hbm, vmem, hbm, vmem, vmem, smem],
        out_specs=[hbm, vmem],
        scratch_shapes=[
            pltpu.VMEM((width, vocab), f32),
            pltpu.VMEM((steps, rows, width), bf16),
            pltpu.VMEM((pieces, n, few, width), bf16),
            pltpu.VMEM((ways, width, vocab), bf16),
            pltpu.VMEM((chunks, n, few, vocab), f32),
            pltpu.VMEM((chunks, n, few, vocab), bf16),
            pltpu.VMEM((ways - 1, chunks, n, few, vocab), bf16),
            pltpu.VMEM((steps, n * rows, LANES), f32),
            pltpu.VMEM((steps, n * rows, LANES), f32),
            pltpu.VMEM((chunks, n * few, LANES), f32),
            pltpu.VMEM((n, 8, rows), jnp.int32),
            pltpu.VMEM((chunks, n, 2, 8, LANES), f32),
            pltpu.VMEM((chunks, 8, LANES), f32),
            pltpu.VMEM((chunks, 8, LANES), f32),
            pltpu.VMEM((chunks, 8, LANES), f32),
            pltpu.VMEM((steps, 8, rows), f32),
            pltpu.VMEM((ways, steps, 8, rows), f32),
            pltpu.VMEM((steps, rows, LANES), f32),
            pltpu.VMEM((ways, chunks, 8, LANES), f32),
            dma((4, pieces, n // 2)),
            dma((pieces, n)),
            dma((chunks, ways - 1)),
            dma((ways - 1,)),
            dma((ways - 1,)),
            dma((ways - 1,)),
            dma((ways - 1,)),
            dma((chunks, n)),
            dma((chunks, n)),
            dma((n,)),
            dma((n,)),
            dma((ways - 1, chunks)),
            dma((ways - 1, chunks)),
            dma((ways - 1,)),
            dma((ways - 1,)),
            dma((2,)),
            dma((width // LANES,)),
        ],
        compiler_params=pltpu.CompilerParams(
            collective_id=7, has_side_effects=True, vmem_limit_bytes=60 * 1024 * 1024
        ),
        name="head_step",
    )(hidden, gain, weight, labels, mask, offsets)


def local(drafter_hidden, norm_gain, head_weight, labels, loss_mask, offsets):
    gradient, loss = head_step(
        drafter_hidden, norm_gain, head_weight, labels[None], loss_mask[None], offsets
    )
    return (loss[0, 0], gradient)


def solution(mesh):
    return jax.shard_map(
        local,
        mesh=mesh,
        in_specs=(P(None, "dp", "tensor"), P("tensor"), P("tensor", "dp"), P("dp"), P("dp"), P()),
        out_specs=(P(), P("tensor", "dp")),
        check_vma=False,
    )
```
